32 devices in a mesh: lat: 4 (over z), lon: 8 (over y, x, core).
Axes of the slice: x: 2, y: 2, z: 4, core: 2. Of those that a mesh axis runs over, the one named last changes fastest.
Arguments:
- zonal_wind: float32 [32, 32, 2048], P(None, 'lat', 'lon'), may hold values from -6 to 6
- merid_wind: float32 [32, 32, 2048], P(None, 'lat', 'lon'), may hold values from -6 to 6
- vertical_wind: float32 [32, 32, 2048], P(None, 'lat', 'lon'), may hold values from -6 to 6
- pressure: float32 [32, 32, 2048], P(None, 'lat', 'lon'), may hold values from -6 to 6
- zonal_coef: float32 [32], P('lat'), may hold values from 0.05 to 0.4
- merid_coef: float32 [32], P('lat'), may hold values from 0.05 to 0.4
- level_coef: float32 [32], replicated, may hold values from 0.3 to 1.5
- sound_coef: float32 [32, 32, 2048], P(None, 'lat', 'lon'), may hold values from 0.2 to 2
- cutoff: int32 [32], replicated, may hold values from 1 to 511
- filter_mask: int32 [32], replicated, may hold values from 0 to 1, as said below
Outputs:
- zonal_next: float32 [32, 32, 2048], P(None, 'lat', 'lon')
- merid_next: float32 [32, 32, 2048], P(None, 'lat', 'lon')
- vertical_next: float32 [32, 32, 2048], P(None, 'lat', 'lon')
- pressure_next: float32 [32, 32, 2048], P(None, 'lat', 'lon')
The draws below stay inside these ranges and needn't reach their ends.
Inputs may be any that keep to these rules, and one draw needn't show every extreme that they name: `filter_mask`: for every latitude j below 16 exactly one of j and j + 16 is filtered; the filtered ones are the first n and the last 16 - n latitudes, for some n from 4 to 12.
All inputs are finite; a program needn't handle non-finite values.
Results may differ from the reference program's by a relative error of at most 0.0001.
Values sent between devices are 32-bit elements; how exact they have to be, the bound alone decides.
A program may use at most 64 MiB of HBM per device.

```python
import math
import jax
import jax.numpy as jnp
from jax import lax

NLON = 2048
NLEV = 32
SUBSTEPS = 2
NLAT = 32


def draw_filter_mask(key, part):
    latitudes = jnp.arange(NLAT)
    northern = jax.random.randint(jax.random.fold_in(key, 17), (), NLAT // 8, 3 * NLAT // 8 + 1)
    southern_start = NLAT // 2 + northern
    return jnp.logical_or(latitudes < northern, latitudes >= southern_start).astype(jnp.int32)


def set_ends(drawn, own_key, smallest, top_value):
    place = [jax.random.randint(jax.random.fold_in(own_key, axis), (), 0, length) for axis, length in enumerate(drawn.shape)]
    widest = drawn.shape.index(max(drawn.shape))
    beside = place[:widest] + [(place[widest] + 1) % drawn.shape[widest]] + place[widest + 1:]
    return drawn.at[tuple(place)].set(smallest).at[tuple(beside)].set(top_value)


def block_scale(stream_key, extent, cuts, low, top_value):
    level = 1.0
    for position, parts in cuts:
        draws = jax.random.uniform(jax.random.fold_in(jax.random.fold_in(stream_key, 6), position), (parts,), jnp.float32, low / len(cuts), top_value / len(cuts))
        level = level * jnp.repeat(jnp.exp(draws), extent[position] // parts).reshape((-1,) + (1,) * (len(extent) - 1 - position))
    return level


def noise(own_key, dims, deviation, reach, shards=(), dtype=jnp.bfloat16):
    entries = deviation * jax.random.normal(own_key, dims, jnp.float32)
    if shards:
        entries = entries * block_scale(own_key, dims, shards, -0.22, 0.18)
    return jnp.clip(entries, -reach, reach).astype(dtype)


def setup_inputs(seed: int = 0) -> dict:
    streams_of = jax.random.split(jax.random.key(seed), 11)
    return {
        "zonal_wind": noise(streams_of[0], (NLEV, NLAT, NLON), 1.0, 6.0, ((1, 4), (2, 8)), jnp.float32),
        "merid_wind": noise(streams_of[1], (NLEV, NLAT, NLON), 1.0, 6.0, ((1, 4), (2, 8)), jnp.float32),
        "vertical_wind": noise(streams_of[2], (NLEV, NLAT, NLON), 1.0, 6.0, ((1, 4), (2, 8)), jnp.float32),
        "pressure": noise(streams_of[3], (NLEV, NLAT, NLON), 1.0, 6.0, ((1, 4), (2, 8)), jnp.float32),
        "zonal_coef": jnp.clip(jnp.exp(math.log(0.4) - 2.0794415 * jax.random.uniform(streams_of[4], (NLAT,), jnp.float32) ** block_scale(streams_of[4], (NLAT,), ((0, 4),), -0.2, 0.2)), 0.05, 0.4),
        "merid_coef": jnp.clip(jnp.exp(math.log(0.4) - 2.0794415 * jax.random.uniform(streams_of[5], (NLAT,), jnp.float32) ** block_scale(streams_of[5], (NLAT,), ((0, 4),), -0.2, 0.2)), 0.05, 0.4),
        "level_coef": jnp.clip(jnp.exp(jax.random.uniform(streams_of[6], (NLEV,), jnp.float32, math.log(0.3), math.log(1.5))), 0.3, 1.5),
        "sound_coef": jnp.clip(jnp.exp(math.log(2.0) - 2.3025851 * jax.random.uniform(streams_of[7], (NLEV, NLAT, NLON), jnp.float32) ** block_scale(streams_of[7], (NLEV, NLAT, NLON), ((1, 4), (2, 8)), -0.2, 0.2)), 0.2, 2.0),
        "cutoff": set_ends(jax.random.randint(streams_of[8], (NLAT,), 1, NLON // 4), jax.random.fold_in(streams_of[8], 1), 1, (NLON // 4) - 1).astype(jnp.int32),
        "filter_mask": draw_filter_mask(jax.random.fold_in(streams_of[10], 71), 0),
    }


def zonal_diff(field):
    return jnp.roll(field, -1, axis=2) - jnp.roll(field, 1, axis=2)


def merid_diff(field):
    padded = jnp.pad(field, ((0, 0), (1, 1), (0, 0)))
    return padded[:, 2:, :] - padded[:, :-2, :]


def damping(wavenum, limits):
    bound_col = limits[:, None]
    ratio = bound_col / jnp.maximum(wavenum[None, :], 1.0)
    return jnp.where(wavenum[None, :] > bound_col, ratio * ratio, 1.0)


def polar_damp(field, cutoff, filter_mask):
    wavenum = jnp.arange(NLON // 2 + 1).astype(jnp.float32)
    factor = damping(wavenum, cutoff.astype(jnp.float32))

    def one_level(slab):
        spectra = jnp.fft.rfft(slab, axis=1)
        return jnp.fft.irfft(spectra * factor, n=NLON, axis=1).astype(jnp.float32)

    damped = lax.map(one_level, field)
    return jnp.where(filter_mask[None, :, None] > 0, damped, field)


def column_solve(vertical_wind, pstar, level_coef, sound_coef):
    levels = vertical_wind.shape[0]
    zero_slab = jnp.zeros_like(vertical_wind[0])
    ratios = []
    values = []
    prev_ratio = zero_slab
    prev_value = zero_slab
    for level in range(levels):
        alpha = level_coef[level]
        below = alpha * sound_coef[level]
        if level + 1 < levels:
            above = alpha * sound_coef[level + 1]
            rhs = vertical_wind[level] - alpha * (pstar[level + 1] - pstar[level])
        else:
            above = zero_slab
            rhs = vertical_wind[level] + alpha * pstar[level]
        pivot = 1.0 + below + above + below * prev_ratio
        prev_ratio = -above / pivot
        prev_value = (rhs + below * prev_value) / pivot
        ratios.append(prev_ratio)
        values.append(prev_value)
    solved = [zero_slab] * levels
    upper_value = values[levels - 1]
    solved[levels - 1] = upper_value
    for level in range(levels - 2, -1, -1):
        upper_value = values[level] - ratios[level] * upper_value
        solved[level] = upper_value
    new_wind = jnp.stack(solved)
    wind_below = jnp.concatenate([zero_slab[None], new_wind[:-1]], axis=0)
    new_pressure = pstar - sound_coef * (new_wind - wind_below)
    return new_wind, new_pressure


def reference(zonal_wind, merid_wind, vertical_wind, pressure, zonal_coef, merid_coef, level_coef, sound_coef, cutoff, filter_mask):
    zonal_rows = zonal_coef[None, :, None]
    merid_rows = merid_coef[None, :, None]
    for step in range(SUBSTEPS):
        zonal_step = -zonal_rows * zonal_diff(pressure)
        merid_step = -merid_rows * merid_diff(pressure)
        zonal_wind = zonal_wind + polar_damp(zonal_step, cutoff, filter_mask)
        merid_wind = merid_wind + polar_damp(merid_step, cutoff, filter_mask)
        diverge = zonal_rows * zonal_diff(zonal_wind) + merid_rows * merid_diff(merid_wind)
        pstar = pressure - sound_coef * diverge
        vertical_wind, pressure = column_solve(vertical_wind, pstar, level_coef, sound_coef)
    return (zonal_wind, merid_wind, vertical_wind, pressure)
```

```python
import functools
import math

import ml_dtypes
import numpy as np
import jax
import jax.numpy as jnp
from jax import lax
from jax.experimental import pallas as pl
from jax.experimental.pallas import tpu as pltpu
from jax.sharding import PartitionSpec as P

SUBSTEPS = 2


def extended(block, sides, width):
    for axis, dim in sides:
        count = lax.axis_size(axis)
        forward = [(i, i + 1) for i in range(count - 1)]
        forward.append((count - 1, 0))
        backward = [(target, source) for source, target in forward]
        low = lax.ppermute(
            lax.slice_in_dim(block, block.shape[dim] - width, None, axis=dim), axis, forward
        )
        high = lax.ppermute(lax.slice_in_dim(block, 0, width, axis=dim), axis, backward)
        block = jnp.concatenate([low, block, high], axis=dim)
    return block


def rim_fix(padded, lat_dim):
    band_index = lax.axis_index("lat")
    bands = lax.axis_size("lat")
    extent = padded.shape[lat_dim]
    position = lax.broadcasted_iota(jnp.int32, padded.shape, lat_dim)
    first_edge = jnp.logical_and(position == 0, band_index == 0)
    final_edge = jnp.logical_and(position == extent - 1, band_index == bands - 1)
    return jnp.where(jnp.logical_or(first_edge, final_edge), 0.0, padded)


def dft_tables(length):
    half_len = length // 2
    sample = lax.broadcasted_iota(jnp.int32, (length, length), 0)
    column = lax.broadcasted_iota(jnp.int32, (length, length), 1)
    is_cosine = column <= half_len
    wavenum = jnp.where(is_cosine, column, column - half_len)
    phase = sample * wavenum % length
    angle = 2.0 * math.pi / length * phase.astype(jnp.float32)
    forward = jnp.where(is_cosine, jnp.cos(angle), jnp.sin(angle))
    single = jnp.logical_and(is_cosine, jnp.logical_or(wavenum == 0, wavenum == half_len))
    weight = jnp.where(single, 1.0, 2.0) / length
    inverse = jnp.transpose(forward * weight)
    wave_row = wavenum[0].astype(jnp.float32)
    return (forward, inverse, wave_row)


def damping(wave_row, limits):
    bound_col = limits[:, None]
    ratio = bound_col / jnp.maximum(wave_row[None, :], 1.0)
    return jnp.where(wave_row[None, :] > bound_col, ratio * ratio, 1.0)


def transform_band(block, limits, forward, inverse, wave_row):
    circles = lax.all_to_all(block, "lon", split_axis=1, concat_axis=3, tiled=True)
    spectra = jnp.einsum("vetj,jc->vetc", circles, forward, precision=lax.Precision.HIGHEST)
    scaled = spectra * damping(wave_row, limits)
    damped = jnp.einsum("vetc,cj->vetj", scaled, inverse, precision=lax.Precision.HIGHEST)
    return lax.all_to_all(damped, "lon", split_axis=3, concat_axis=1, tiled=True)


def filtered_increments(increments, own_flags, own_limits, forward, inverse, wave_row):
    flag_cols = own_flags[:, None]
    damped = transform_band(increments, own_limits, forward, inverse, wave_row)
    return jnp.where(flag_cols, damped, increments)


def column_solve(vertical_wind, pstar, level_coef, sound_coef):
    levels = vertical_wind.shape[0]
    zero_slab = jnp.zeros_like(vertical_wind[0])
    ratios = []
    values = []
    prev_ratio = zero_slab
    prev_value = zero_slab
    for level in range(levels):
        alpha = level_coef[level]
        below = alpha * sound_coef[level]
        if level + 1 < levels:
            above = alpha * sound_coef[level + 1]
            rhs = vertical_wind[level] - alpha * (pstar[level + 1] - pstar[level])
        else:
            above = zero_slab
            rhs = vertical_wind[level] + alpha * pstar[level]
        pivot = 1.0 + below + above + below * prev_ratio
        prev_ratio = -above / pivot
        prev_value = (rhs + below * prev_value) / pivot
        ratios.append(prev_ratio)
        values.append(prev_value)
    solved = [zero_slab] * levels
    upper_value = values[levels - 1]
    solved[levels - 1] = upper_value
    for level in range(levels - 2, -1, -1):
        upper_value = values[level] - ratios[level] * upper_value
        solved[level] = upper_value
    new_wind = jnp.stack(solved)
    wind_below = jnp.concatenate([zero_slab[None], new_wind[:-1]], axis=0)
    new_pressure = pstar - sound_coef * (new_wind - wind_below)
    return (new_wind, new_pressure)


def wide_body(
    zonal_wind,
    merid_wind,
    vertical_wind,
    pressure,
    zonal_coef,
    merid_coef,
    level_coef,
    sound_coef,
    cutoff,
    filter_mask,
):
    lat_rows = pressure.shape[1]
    start = lax.axis_index("lat") * lat_rows
    own_flags = lax.dynamic_slice_in_dim(filter_mask, start, lat_rows) > 0
    own_limits = lax.dynamic_slice_in_dim(cutoff, start, lat_rows).astype(jnp.float32)
    forward, inverse, wave_row = dft_tables(pressure.shape[2] * lax.axis_size("lon"))
    zonal_rows = zonal_coef[None, :, None]
    merid_rows = merid_coef[None, :, None]
    for step in range(SUBSTEPS):
        padded = extended(pressure, (("lat", 1), ("lon", 2)), 1)
        padded = rim_fix(padded, 1)
        zonal_step = -zonal_rows * (padded[:, 1:-1, 2:] - padded[:, 1:-1, :-2])
        merid_step = -merid_rows * (padded[:, 2:, 1:-1] - padded[:, :-2, 1:-1])
        increments = jnp.stack([zonal_step, merid_step])
        damped = filtered_increments(increments, own_flags, own_limits, forward, inverse, wave_row)
        winds = jnp.stack([zonal_wind, merid_wind]) + damped
        wind_pad = extended(winds, (("lat", 2), ("lon", 3)), 1)
        wind_pad = rim_fix(wind_pad, 2)
        diverge = zonal_rows * (wind_pad[0, :, 1:-1, 2:] - wind_pad[0, :, 1:-1, :-2])
        diverge = diverge + merid_rows * (wind_pad[1, :, 2:, 1:-1] - wind_pad[1, :, :-2, 1:-1])
        pstar = pressure - sound_coef * diverge
        vertical_wind, pressure = column_solve(vertical_wind, pstar, level_coef, sound_coef)
        zonal_wind = winds[0]
        merid_wind = winds[1]
    return (zonal_wind, merid_wind, vertical_wind, pressure)


LANE = 128
TILE = 2 * LANE


def circle_tables(length):
    blocks = length // LANE
    half = blocks // 2
    m = np.arange(LANE, dtype=np.float64)[:, None]
    tables = np.zeros((half, TILE, TILE))
    waves = np.zeros((half, TILE))
    c = np.arange(LANE)[None, :]
    low = np.where(c <= LANE // 2, np.cos(2 * np.pi * m * c / LANE), np.sin(2 * np.pi * m * (c - LANE // 2) / LANE))
    low = low * np.where((c == 0) | (c == LANE // 2), np.sqrt(1.0 / LANE), np.sqrt(2.0 / LANE))
    k2 = np.arange(LANE // 2)[None, :]
    angle = 2 * np.pi * m * (half + blocks * k2) / length
    mid = np.concatenate([np.cos(angle), np.sin(angle)], axis=1) * np.sqrt(2.0 / LANE)
    tables[0, :LANE, :LANE] = low
    tables[0, LANE:, LANE:] = mid
    waves[0, :LANE] = blocks * np.where(c[0] <= LANE // 2, c[0], c[0] - LANE // 2)
    waves[0, LANE:] = np.tile(half + blocks * k2[0], 2)
    for k1 in range(1, half):
        k = k1 + blocks * c
        angle = 2 * np.pi * ((m * k) % length) / length
        cos, sin = np.cos(angle) / np.sqrt(LANE), np.sin(angle) / np.sqrt(LANE)
        tables[k1] = np.block([[cos, -sin], [sin, cos]])
        waves[k1] = np.tile(np.minimum(k[0], length - k[0]), 2)
    high = tables.astype(ml_dtypes.bfloat16)
    rest = (tables - high.astype(np.float64)).astype(ml_dtypes.bfloat16)
    scale = np.full((half, TILE), 2.0 / blocks)
    scale[0] = 1.0 / blocks
    rows = np.zeros((8, half * TILE), np.float32)
    rows[0] = waves.reshape(-1)
    rows[1] = (4.0 * np.sin(2 * np.pi * waves / length) ** 2).reshape(-1)
    rows[2] = scale.reshape(-1)
    return high, rest, rows


def split_parts(value):
    high = value.astype(jnp.bfloat16)
    rest = (value - high.astype(jnp.float32)).astype(jnp.bfloat16)
    return high, rest


def three_products(value, high_table, rest_table, transposed):
    high, rest = split_parts(value)
    dims = (((1,), (1 if transposed else 0,)), ((), ()))
    rows = value.shape[0]
    both = lax.dot_general(jnp.concatenate([high, rest], axis=0), high_table, dims, preferred_element_type=jnp.float32)
    corr = lax.dot_general(high, rest_table, dims, preferred_element_type=jnp.float32)
    return both[:rows] + (both[rows:] + corr)


def weighted(terms):
    total = None
    for coef, value in terms:
        if abs(coef) < 1e-12:
            continue
        if abs(abs(coef) - 1.0) < 1e-12:
            term = value
        else:
            term = abs(coef) * value
        if total is None:
            total = term if coef > 0 else -term
        else:
            total = total + term if coef > 0 else total - term
    return total


def coarse_forward(xs):
    count = len(xs)
    half = count // 2
    even = {b: xs[b] + xs[count - b] for b in range(1, half)}
    odd = {b: xs[b] - xs[count - b] for b in range(1, half)}
    real, imag = [], {}
    for k in range(half + 1):
        ends = xs[0] + xs[half] if k % 2 == 0 else xs[0] - xs[half]
        real.append(weighted([(1.0, ends)] + [(math.cos(2 * math.pi * b * k / count), even[b]) for b in range(1, half)]))
    for k in range(1, half):
        imag[k] = weighted([(-math.sin(2 * math.pi * b * k / count), odd[b]) for b in range(1, half)])
    pairs = [(real[0], real[half])] + [(real[k], imag[k]) for k in range(1, half)]
    return pairs


def coarse_inverse(pairs):
    half = len(pairs)
    count = 2 * half
    first, last = pairs[0]
    xs = [None] * count
    for b in range(half + 1):
        ends = first + last if b % 2 == 0 else first - last
        cos_part = weighted([(1.0, ends)] + [(math.cos(2 * math.pi * b * k / count), pairs[k][0]) for k in range(1, half)])
        if b in (0, half):
            xs[b] = cos_part
        else:
            sin_part = weighted([(-math.sin(2 * math.pi * b * k / count), pairs[k][1]) for k in range(1, half)])
            xs[b] = cos_part + sin_part
            xs[count - b] = cos_part - sin_part
    return xs


def to_spectrum(x_ref, high_ref, rest_ref, work_ref, spec_ref, bands, per_band, add_ref=None):
    rows = x_ref.shape[1]
    split = x_ref.shape[2] // LANE
    for band in range(bands):
        xs = [
            x_ref[band * per_band + d, :, h * LANE:(h + 1) * LANE]
            for d in range(per_band)
            for h in range(split)
        ]
        for t, (left, right) in enumerate(coarse_forward(xs)):
            work_ref[band * rows:(band + 1) * rows, t * TILE:t * TILE + LANE] = left
            work_ref[band * rows:(band + 1) * rows, t * TILE + LANE:(t + 1) * TILE] = right
    for t in range(high_ref.shape[0]):
        cols = slice(t * TILE, (t + 1) * TILE)
        value = three_products(work_ref[:, cols], high_ref[t], rest_ref[t], False)
        if add_ref is not None:
            value = value + add_ref[:, cols]
        spec_ref[:, cols] = value


def lat_diff(value):
    count = value.shape[0]
    row = lax.broadcasted_iota(jnp.int32, value.shape, 0)
    upper = jnp.where(row == count - 1, 0.0, pltpu.roll(value, count - 1, 0))
    lower = jnp.where(row == 0, 0.0, pltpu.roll(value, 1, 0))
    return upper - lower


def filter_rows(rows_ref, cols, cols_ref):
    wave = rows_ref[0:1, cols]
    limit = cols_ref[:, 2:3]
    ratio = limit / jnp.maximum(wave, 1.0)
    damped = jnp.logical_and(wave > limit, cols_ref[:, 3:4] > 0)
    return jnp.where(damped, ratio * ratio, 1.0)


def circle_blocks(work_ref, band, rows, half):
    span = slice(band * rows, (band + 1) * rows)
    pairs = [
        (work_ref[span, t * TILE:t * TILE + LANE], work_ref[span, t * TILE + LANE:(t + 1) * TILE])
        for t in range(half)
    ]
    return coarse_inverse(pairs)


def put_blocks(out_ref, xs, band, per_band):
    split = out_ref.shape[2] // LANE
    for b, value in enumerate(xs):
        out_ref[band * per_band + b // split, :, (b % split) * LANE:(b % split + 1) * LANE] = value


def circle_diff(xs):
    count = len(xs)
    lane = lax.broadcasted_iota(jnp.int32, xs[0].shape, 1)
    ahead = [pltpu.roll(x, LANE - 1, 1) for x in xs]
    behind = [pltpu.roll(x, 1, 1) for x in xs]
    out = []
    for b in range(count):
        nxt = jnp.where(lane == LANE - 1, ahead[(b + 1) % count], ahead[b])
        prv = jnp.where(lane == 0, behind[(b - 1) % count], behind[b])
        out.append(nxt - prv)
    return out


def spectral_terms(spec, rows_ref, cols_ref, cols):
    zonal = cols_ref[:, 0:1]
    merid = cols_ref[:, 1:2]
    factor = filter_rows(rows_ref, cols, cols_ref) * rows_ref[2:3, cols]
    smooth = factor * spec
    v_part = -(merid * factor) * lat_diff(spec)
    d_part = (zonal * zonal) * rows_ref[1:2, cols] * smooth + merid * lat_diff(v_part)
    return smooth, v_part, d_part


def divergence_kernel(bands, per_band, x_ref, high_ref, rest_ref, rows_ref, cols_ref, d_ref, spec_ref, work_ref):
    half = high_ref.shape[0]
    rows = x_ref.shape[1]
    to_spectrum(x_ref, high_ref, rest_ref, work_ref, spec_ref, bands, per_band)
    for t in range(half):
        cols = slice(t * TILE, (t + 1) * TILE)
        _, _, d_part = spectral_terms(spec_ref[:, cols], rows_ref, cols_ref, cols)
        work_ref[:, cols] = three_products(d_part, high_ref[t], rest_ref[t], True)
    for band in range(bands):
        put_blocks(d_ref, circle_blocks(work_ref, band, rows, half), band, per_band)


def final_kernel(bands, per_band, x_ref, old_ref, high_ref, rest_ref, rows_ref, cols_ref, d_ref, u_ref, v_ref, spec_ref, work_ref, q_ref, v_work_ref):
    half = high_ref.shape[0]
    rows = x_ref.shape[1]
    lats = old_ref.shape[0]
    to_spectrum(x_ref, high_ref, rest_ref, work_ref, spec_ref, bands, per_band, old_ref)
    for t in range(half):
        cols = slice(t * TILE, (t + 1) * TILE)
        smooth, v_part, d_part = spectral_terms(spec_ref[:, cols], rows_ref, cols_ref, cols)
        value = three_products(jnp.concatenate([d_part, smooth, v_part], axis=0), high_ref[t], rest_ref[t], True)
        work_ref[:, cols] = value[:lats]
        q_ref[:, cols] = value[lats:2 * lats]
        v_work_ref[:, cols] = value[2 * lats:]
    for band in range(bands):
        put_blocks(d_ref, circle_blocks(work_ref, band, rows, half), band, per_band)
        put_blocks(v_ref, circle_blocks(v_work_ref, band, rows, half), band, per_band)
        zonal = cols_ref[band * rows:(band + 1) * rows, 0:1]
        moved = circle_diff(circle_blocks(q_ref, band, rows, half))
        put_blocks(u_ref, [-zonal * x for x in moved], band, per_band)


def factor_columns(a_ref, s_ref, ratio_ref, inv_ref):
    levels = s_ref.shape[0]
    prev = jnp.zeros(s_ref.shape[1:], jnp.float32)
    for level in range(levels):
        alpha = a_ref[level]
        below = alpha * s_ref[level]
        above = alpha * s_ref[level + 1] if level + 1 < levels else jnp.zeros_like(below)
        inv = 1.0 / (1.0 + below + above + below * prev)
        prev = -above * inv
        ratio_ref[level] = prev
        inv_ref[level] = inv


def solve_columns(a_ref, s_ref, w_ref, p_ref, base_ref, d_ref, ratio_ref, inv_ref, w_out, p_out):
    levels = s_ref.shape[0]

    def star(level):
        return p_ref[level] - s_ref[level] * (base_ref[level] + d_ref[level])

    here = star(0)
    prev = jnp.zeros_like(here)
    for level in range(levels):
        alpha = a_ref[level]
        p_out[level] = here
        if level + 1 < levels:
            nxt = star(level + 1)
            rhs = w_ref[level] - alpha * (nxt - here)
        else:
            nxt = here
            rhs = w_ref[level] + alpha * here
        prev = (rhs + alpha * s_ref[level] * prev) * inv_ref[level]
        w_out[level] = prev
        here = nxt
    upper = w_out[levels - 1]
    for level in range(levels - 1, 0, -1):
        lower = w_out[level - 1] - ratio_ref[level - 1] * upper
        w_out[level - 1] = lower
        p_out[level] = p_out[level] - s_ref[level] * (upper - lower)
        upper = lower
    p_out[0] = p_out[0] - s_ref[0] * upper


def first_column_kernel(a_ref, s_ref, w_ref, p_ref, base_ref, d_ref, w_out, p_out, ratio_ref, inv_ref):
    factor_columns(a_ref, s_ref, ratio_ref, inv_ref)
    solve_columns(a_ref, s_ref, w_ref, p_ref, base_ref, d_ref, ratio_ref, inv_ref, w_out, p_out)


def last_column_kernel(a_ref, s_ref, w_ref, p_ref, base_ref, d_ref, ratio_ref, inv_ref, u_ref, v_ref, du_ref, dv_ref, u_out, v_out, w_out, p_out):
    u_out[...] = u_ref[...] + du_ref[...]
    v_out[...] = v_ref[...] + dv_ref[...]
    solve_columns(a_ref, s_ref, w_ref, p_ref, base_ref, d_ref, ratio_ref, inv_ref, w_out, p_out)


def level_body(
    tables,
    zonal_wind,
    merid_wind,
    vertical_wind,
    pressure,
    zonal_coef,
    merid_coef,
    level_coef,
    sound_coef,
    cutoff,
    filter_mask,
):
    high, rest, rows = (jnp.asarray(t) for t in tables)
    bands = lax.axis_size("lat")
    per_band = lax.axis_size("lon")
    lats = cutoff.shape[0]
    both = lax.all_gather(jnp.stack([zonal_coef, merid_coef], axis=1), "lat", axis=0, tiled=True)
    cols = jnp.concatenate([both, cutoff.astype(jnp.float32)[:, None], filter_mask.astype(jnp.float32)[:, None]], axis=1)
    zonal_rows = zonal_coef[None, :, None]
    merid_rows = merid_coef[None, :, None]
    u_pad = extended(zonal_wind, (("lon", 2),), 1)
    v_pad = rim_fix(extended(merid_wind, (("lat", 1),), 1), 1)
    base = zonal_rows * (u_pad[:, :, 2:] - u_pad[:, :, :-2]) + merid_rows * (v_pad[:, 2:] - v_pad[:, :-2])

    def swap(block):
        return lax.all_to_all(block, ("lat", "lon"), split_axis=0, concat_axis=0, tiled=True)

    vmem = pl.BlockSpec(memory_space=pltpu.VMEM)
    smem = pl.BlockSpec(memory_space=pltpu.SMEM)
    block = jax.ShapeDtypeStruct(pressure.shape, jnp.float32)
    flat = jax.ShapeDtypeStruct((lats, rows.shape[1]), jnp.float32)
    scratch = pltpu.VMEM(flat.shape, jnp.float32)

    div, spec = pl.pallas_call(
        functools.partial(divergence_kernel, bands, per_band),
        out_shape=(block, flat), in_specs=[vmem] * 5, out_specs=(vmem, vmem), scratch_shapes=[scratch],
    )(swap(pressure), high, rest, rows, cols)
    w_mid, p_mid, ratio, inv = pl.pallas_call(
        first_column_kernel,
        out_shape=(block,) * 4, in_specs=[smem] + [vmem] * 5, out_specs=(vmem,) * 4,
    )(level_coef, sound_coef, vertical_wind, pressure, base, swap(div))
    div, du, dv = pl.pallas_call(
        functools.partial(final_kernel, bands, per_band),
        out_shape=(block,) * 3, in_specs=[vmem] * 6, out_specs=(vmem,) * 3, scratch_shapes=[scratch] * 4,
    )(swap(p_mid), spec, high, rest, rows, cols)
    return pl.pallas_call(
        last_column_kernel,
        out_shape=(block,) * 4, in_specs=[smem] + [vmem] * 11, out_specs=(vmem,) * 4,
    )(level_coef, sound_coef, w_mid, p_mid, base, swap(div), ratio, inv, zonal_wind, merid_wind, swap(du), swap(dv))


def body(tables, *arrays):
    pressure = arrays[3]
    devices = lax.axis_size("lat") * lax.axis_size("lon")
    fits = pressure.shape[0] == devices and pressure.shape[1] % 8 == 0 and pressure.shape[2] % LANE == 0
    if fits:
        return level_body(tables, *arrays)
    return wide_body(*arrays)


def solution(mesh):
    in_specs = (
        P(None, "lat", "lon"),
        P(None, "lat", "lon"),
        P(None, "lat", "lon"),
        P(None, "lat", "lon"),
        P("lat"),
        P("lat"),
        P(),
        P(None, "lat", "lon"),
        P(),
        P(),
    )
    out_specs = (
        P(None, "lat", "lon"),
        P(None, "lat", "lon"),
        P(None, "lat", "lon"),
        P(None, "lat", "lon"),
    )

    def whole(*arrays):
        tables = circle_tables(arrays[0].shape[2])
        step = jax.shard_map(functools.partial(body, tables), mesh=mesh, in_specs=in_specs, out_specs=out_specs, check_vma=False)
        return step(*arrays)

    return whole
```

```python
import functools
import math

import ml_dtypes
import numpy as np
import jax
import jax.numpy as jnp
from jax import lax
from jax.experimental import pallas as pl
from jax.experimental.pallas import tpu as pltpu
from jax.sharding import PartitionSpec as P

SUBSTEPS = 2


def extended(block, sides, width):
    for axis, dim in sides:
        count = lax.axis_size(axis)
        forward = [(i, i + 1) for i in range(count - 1)]
        forward.append((count - 1, 0))
        backward = [(target, source) for source, target in forward]
        low = lax.ppermute(
            lax.slice_in_dim(block, block.shape[dim] - width, None, axis=dim), axis, forward
        )
        high = lax.ppermute(lax.slice_in_dim(block, 0, width, axis=dim), axis, backward)
        block = jnp.concatenate([low, block, high], axis=dim)
    return block


def rim_fix(padded, lat_dim):
    band_index = lax.axis_index("lat")
    bands = lax.axis_size("lat")
    extent = padded.shape[lat_dim]
    position = lax.broadcasted_iota(jnp.int32, padded.shape, lat_dim)
    first_edge = jnp.logical_and(position == 0, band_index == 0)
    final_edge = jnp.logical_and(position == extent - 1, band_index == bands - 1)
    return jnp.where(jnp.logical_or(first_edge, final_edge), 0.0, padded)


def dft_tables(length):
    half_len = length // 2
    sample = lax.broadcasted_iota(jnp.int32, (length, length), 0)
    column = lax.broadcasted_iota(jnp.int32, (length, length), 1)
    is_cosine = column <= half_len
    wavenum = jnp.where(is_cosine, column, column - half_len)
    phase = sample * wavenum % length
    angle = 2.0 * math.pi / length * phase.astype(jnp.float32)
    forward = jnp.where(is_cosine, jnp.cos(angle), jnp.sin(angle))
    single = jnp.logical_and(is_cosine, jnp.logical_or(wavenum == 0, wavenum == half_len))
    weight = jnp.where(single, 1.0, 2.0) / length
    inverse = jnp.transpose(forward * weight)
    wave_row = wavenum[0].astype(jnp.float32)
    return (forward, inverse, wave_row)


def damping(wave_row, limits):
    bound_col = limits[:, None]
    ratio = bound_col / jnp.maximum(wave_row[None, :], 1.0)
    return jnp.where(wave_row[None, :] > bound_col, ratio * ratio, 1.0)


def transform_band(block, limits, forward, inverse, wave_row):
    circles = lax.all_to_all(block, "lon", split_axis=1, concat_axis=3, tiled=True)
    spectra = jnp.einsum("vetj,jc->vetc", circles, forward, precision=lax.Precision.HIGHEST)
    scaled = spectra * damping(wave_row, limits)
    damped = jnp.einsum("vetc,cj->vetj", scaled, inverse, precision=lax.Precision.HIGHEST)
    return lax.all_to_all(damped, "lon", split_axis=3, concat_axis=1, tiled=True)


def filtered_increments(increments, own_flags, own_limits, forward, inverse, wave_row):
    flag_cols = own_flags[:, None]
    damped = transform_band(increments, own_limits, forward, inverse, wave_row)
    return jnp.where(flag_cols, damped, increments)


def column_solve(vertical_wind, pstar, level_coef, sound_coef):
    levels = vertical_wind.shape[0]
    zero_slab = jnp.zeros_like(vertical_wind[0])
    ratios = []
    values = []
    prev_ratio = zero_slab
    prev_value = zero_slab
    for level in range(levels):
        alpha = level_coef[level]
        below = alpha * sound_coef[level]
        if level + 1 < levels:
            above = alpha * sound_coef[level + 1]
            rhs = vertical_wind[level] - alpha * (pstar[level + 1] - pstar[level])
        else:
            above = zero_slab
            rhs = vertical_wind[level] + alpha * pstar[level]
        pivot = 1.0 + below + above + below * prev_ratio
        prev_ratio = -above / pivot
        prev_value = (rhs + below * prev_value) / pivot
        ratios.append(prev_ratio)
        values.append(prev_value)
    solved = [zero_slab] * levels
    upper_value = values[levels - 1]
    solved[levels - 1] = upper_value
    for level in range(levels - 2, -1, -1):
        upper_value = values[level] - ratios[level] * upper_value
        solved[level] = upper_value
    new_wind = jnp.stack(solved)
    wind_below = jnp.concatenate([zero_slab[None], new_wind[:-1]], axis=0)
    new_pressure = pstar - sound_coef * (new_wind - wind_below)
    return (new_wind, new_pressure)


def wide_body(
    zonal_wind,
    merid_wind,
    vertical_wind,
    pressure,
    zonal_coef,
    merid_coef,
    level_coef,
    sound_coef,
    cutoff,
    filter_mask,
):
    lat_rows = pressure.shape[1]
    start = lax.axis_index("lat") * lat_rows
    own_flags = lax.dynamic_slice_in_dim(filter_mask, start, lat_rows) > 0
    own_limits = lax.dynamic_slice_in_dim(cutoff, start, lat_rows).astype(jnp.float32)
    forward, inverse, wave_row = dft_tables(pressure.shape[2] * lax.axis_size("lon"))
    zonal_rows = zonal_coef[None, :, None]
    merid_rows = merid_coef[None, :, None]
    for step in range(SUBSTEPS):
        padded = extended(pressure, (("lat", 1), ("lon", 2)), 1)
        padded = rim_fix(padded, 1)
        zonal_step = -zonal_rows * (padded[:, 1:-1, 2:] - padded[:, 1:-1, :-2])
        merid_step = -merid_rows * (padded[:, 2:, 1:-1] - padded[:, :-2, 1:-1])
        increments = jnp.stack([zonal_step, merid_step])
        damped = filtered_increments(increments, own_flags, own_limits, forward, inverse, wave_row)
        winds = jnp.stack([zonal_wind, merid_wind]) + damped
        wind_pad = extended(winds, (("lat", 2), ("lon", 3)), 1)
        wind_pad = rim_fix(wind_pad, 2)
        diverge = zonal_rows * (wind_pad[0, :, 1:-1, 2:] - wind_pad[0, :, 1:-1, :-2])
        diverge = diverge + merid_rows * (wind_pad[1, :, 2:, 1:-1] - wind_pad[1, :, :-2, 1:-1])
        pstar = pressure - sound_coef * diverge
        vertical_wind, pressure = column_solve(vertical_wind, pstar, level_coef, sound_coef)
        zonal_wind = winds[0]
        merid_wind = winds[1]
    return (zonal_wind, merid_wind, vertical_wind, pressure)


LANE = 128
TILE = 2 * LANE


def circle_tables(length):
    blocks = length // LANE
    half = blocks // 2
    m = np.arange(LANE, dtype=np.float64)[:, None]
    tables = np.zeros((half, TILE, TILE))
    waves = np.zeros((half, TILE))
    c = np.arange(LANE)[None, :]
    low = np.where(c <= LANE // 2, np.cos(2 * np.pi * m * c / LANE), np.sin(2 * np.pi * m * (c - LANE // 2) / LANE))
    low = low * np.where((c == 0) | (c == LANE // 2), np.sqrt(1.0 / LANE), np.sqrt(2.0 / LANE))
    k2 = np.arange(LANE // 2)[None, :]
    angle = 2 * np.pi * m * (half + blocks * k2) / length
    mid = np.concatenate([np.cos(angle), np.sin(angle)], axis=1) * np.sqrt(2.0 / LANE)
    tables[0, :LANE, :LANE] = low
    tables[0, LANE:, LANE:] = mid
    waves[0, :LANE] = blocks * np.where(c[0] <= LANE // 2, c[0], c[0] - LANE // 2)
    waves[0, LANE:] = np.tile(half + blocks * k2[0], 2)
    for k1 in range(1, half):
        k = k1 + blocks * c
        angle = 2 * np.pi * ((m * k) % length) / length
        cos, sin = np.cos(angle) / np.sqrt(LANE), np.sin(angle) / np.sqrt(LANE)
        tables[k1] = np.block([[cos, -sin], [sin, cos]])
        waves[k1] = np.tile(np.minimum(k[0], length - k[0]), 2)
    high = tables.astype(ml_dtypes.bfloat16)
    rest = (tables - high.astype(np.float64)).astype(ml_dtypes.bfloat16)
    scale = np.full((half, TILE), 2.0 / blocks)
    scale[0] = 1.0 / blocks
    rows = np.zeros((half, 8, TILE), np.float32)
    rows[:, 0] = waves
    rows[:, 1] = 4.0 * np.sin(2 * np.pi * waves / length) ** 2
    rows[:, 2] = scale
    return high, rest, rows


def split_parts(value):
    high = value.astype(jnp.bfloat16)
    rest = (value - high.astype(jnp.float32)).astype(jnp.bfloat16)
    return high, rest


def three_products(value, high_table, rest_table, transposed):
    high, rest = split_parts(value)
    dims = (((1,), (1 if transposed else 0,)), ((), ()))
    rows = value.shape[0]
    both = lax.dot_general(jnp.concatenate([high, rest], axis=0), high_table, dims, preferred_element_type=jnp.float32)
    corr = lax.dot_general(high, rest_table, dims, preferred_element_type=jnp.float32)
    return both[:rows] + (both[rows:] + corr)


def weighted(terms):
    total = None
    for coef, value in terms:
        if abs(coef) < 1e-12:
            continue
        if abs(abs(coef) - 1.0) < 1e-12:
            term = value
        else:
            term = abs(coef) * value
        if total is None:
            total = term if coef > 0 else -term
        else:
            total = total + term if coef > 0 else total - term
    return total


def coarse_forward(xs):
    count = len(xs)
    half = count // 2
    even = {b: xs[b] + xs[count - b] for b in range(1, half)}
    odd = {b: xs[b] - xs[count - b] for b in range(1, half)}
    real, imag = [], {}
    for k in range(half + 1):
        ends = xs[0] + xs[half] if k % 2 == 0 else xs[0] - xs[half]
        real.append(weighted([(1.0, ends)] + [(math.cos(2 * math.pi * b * k / count), even[b]) for b in range(1, half)]))
    for k in range(1, half):
        imag[k] = weighted([(-math.sin(2 * math.pi * b * k / count), odd[b]) for b in range(1, half)])
    pairs = [(real[0], real[half])] + [(real[k], imag[k]) for k in range(1, half)]
    return pairs


def coarse_inverse(pairs):
    half = len(pairs)
    count = 2 * half
    first, last = pairs[0]
    xs = [None] * count
    for b in range(half + 1):
        ends = first + last if b % 2 == 0 else first - last
        cos_part = weighted([(1.0, ends)] + [(math.cos(2 * math.pi * b * k / count), pairs[k][0]) for k in range(1, half)])
        if b in (0, half):
            xs[b] = cos_part
        else:
            sin_part = weighted([(-math.sin(2 * math.pi * b * k / count), pairs[k][1]) for k in range(1, half)])
            xs[b] = cos_part + sin_part
            xs[count - b] = cos_part - sin_part
    return xs


def to_spectrum(x_ref, high_ref, rest_ref, work_ref, spec_ref, bands, per_band, accumulate):
    split = x_ref.shape[2] // LANE

    def one_band(band, carry):
        xs = [
            x_ref[band * per_band + d, :, h * LANE:(h + 1) * LANE]
            for d in range(per_band)
            for h in range(split)
        ]
        for t, (left, right) in enumerate(coarse_forward(xs)):
            work_ref[t, band, :, :LANE] = left
            work_ref[t, band, :, LANE:] = right
        return carry

    lax.fori_loop(0, bands, one_band, 0)
    for t in range(high_ref.shape[0]):
        value = three_products(joined(work_ref[t]), high_ref[t], rest_ref[t], False)
        if accumulate:
            value = value + spec_ref[t]
        spec_ref[t] = value


def joined(value):
    return value.reshape((value.shape[0] * value.shape[1], value.shape[2]))


def lat_diff(value):
    count = value.shape[0]
    row = lax.broadcasted_iota(jnp.int32, value.shape, 0)
    upper = jnp.where(row == count - 1, 0.0, pltpu.roll(value, count - 1, 0))
    lower = jnp.where(row == 0, 0.0, pltpu.roll(value, 1, 0))
    return upper - lower


def circle_blocks(work_ref, band):
    pairs = [(work_ref[t, band, :, :LANE], work_ref[t, band, :, LANE:]) for t in range(work_ref.shape[0])]
    return coarse_inverse(pairs)


def put_blocks(out_ref, xs, band, per_band):
    split = out_ref.shape[2] // LANE
    for b, value in enumerate(xs):
        out_ref[band * per_band + b // split, :, (b % split) * LANE:(b % split + 1) * LANE] = value


def circle_diff(xs):
    count = len(xs)
    lane = lax.broadcasted_iota(jnp.int32, xs[0].shape, 1)
    ahead = [pltpu.roll(x, LANE - 1, 1) for x in xs]
    behind = [pltpu.roll(x, 1, 1) for x in xs]
    out = []
    for b in range(count):
        nxt = jnp.where(lane == LANE - 1, ahead[(b + 1) % count], ahead[b])
        prv = jnp.where(lane == 0, behind[(b - 1) % count], behind[b])
        out.append(nxt - prv)
    return out


def spectral_terms(spec, factor, sines, coef_ref):
    coefs = coef_ref[...]
    zonal = joined(coefs[:, 0])[:, 0:1]
    merid = joined(coefs[:, 1])[:, 0:1]
    smooth = factor * spec
    v_part = -(merid * factor) * lat_diff(spec)
    d_part = (zonal * zonal) * sines * smooth + merid * lat_diff(v_part)
    return smooth, v_part, d_part


def factor_columns(a_ref, s_ref, ratio_ref, inv_ref):
    levels = s_ref.shape[0]
    prev = jnp.zeros(s_ref.shape[1:], jnp.float32)
    for level in range(levels):
        alpha = a_ref[level]
        below = alpha * s_ref[level]
        above = alpha * s_ref[level + 1] if level + 1 < levels else jnp.zeros_like(below)
        inv = 1.0 / (1.0 + below + above + below * prev)
        prev = -above * inv
        ratio_ref[level] = prev
        inv_ref[level] = inv


def solve_columns(a_ref, s_ref, w_ref, p_ref, base_ref, d_ref, ratio_ref, inv_ref, w_out, p_out):
    levels = s_ref.shape[0]

    def star(level):
        return p_ref[level] - s_ref[level] * (base_ref[level] + d_ref[level])

    here = star(0)
    prev = jnp.zeros_like(here)
    for level in range(levels):
        alpha = a_ref[level]
        p_out[level] = here
        if level + 1 < levels:
            nxt = star(level + 1)
            rhs = w_ref[level] - alpha * (nxt - here)
        else:
            nxt = here
            rhs = w_ref[level] + alpha * here
        prev = (rhs + alpha * s_ref[level] * prev) * inv_ref[level]
        w_out[level] = prev
        here = nxt
    upper = w_out[levels - 1]
    for level in range(levels - 1, 0, -1):
        lower = w_out[level - 1] - ratio_ref[level - 1] * upper
        w_out[level - 1] = lower
        p_out[level] = p_out[level] - s_ref[level] * (upper - lower)
        upper = lower
    p_out[0] = p_out[0] - s_ref[0] * upper


def base_divergence(u_ref, v_ref, own_ref, west_ref, east_ref, south_ref, north_ref, base_ref, is_first, is_last):
    zonal = own_ref[0][:, 0:1]
    merid = own_ref[1][:, 0:1]
    rows, width = u_ref.shape[1:]
    lane = lax.broadcasted_iota(jnp.int32, (rows, width), 1)
    row = lax.broadcasted_iota(jnp.int32, (rows, width), 0)
    keep_south = jnp.where(is_first, 0.0, 1.0)
    keep_north = jnp.where(is_last, 0.0, 1.0)
    west = west_ref[...]
    east = east_ref[...]
    for level in range(u_ref.shape[0]):
        u = u_ref[level]
        v = v_ref[level]
        ahead = jnp.where(lane == width - 1, east[:, level:level + 1], pltpu.roll(u, width - 1, 1))
        behind = jnp.where(lane == 0, west[:, level:level + 1], pltpu.roll(u, 1, 1))
        upper = jnp.where(row == rows - 1, keep_north * north_ref[level:level + 1, :], pltpu.roll(v, rows - 1, 0))
        lower = jnp.where(row == 0, keep_south * south_ref[level:level + 1, :], pltpu.roll(v, 1, 0))
        base_ref[level] = zonal * (ahead - behind) + merid * (upper - lower)


def pack_edges(u_ref, v_ref, first_col, last_col, first_row, last_row):
    rows, width = u_ref.shape[1:]
    lane = lax.broadcasted_iota(jnp.int32, (rows, LANE), 1)
    first = jnp.zeros((rows, LANE), jnp.float32)
    last = jnp.zeros((rows, LANE), jnp.float32)
    for level in range(u_ref.shape[0]):
        first = jnp.where(lane == level, u_ref[level, :, 0:1], first)
        last = jnp.where(lane == level, u_ref[level, :, width - 1:width], last)
        first_row[level:level + 1, :] = v_ref[level, 0:1, :]
        last_row[level:level + 1, :] = v_ref[level, rows - 1:rows, :]
    first_col[...] = first
    last_col[...] = last


def fused_kernel(
    bands, per_band, a_ref, u_ref, v_ref, w_ref, p_ref, s_ref, own_ref, limit_ref, high_ref, rest_ref, rows_ref,
    u_out, v_out, w_out, p_out,
    x1, d1, x2, d2, ur, vr, ds1, ds2, us, vs, w_mid, p_mid, base, ratio, inv,
    work, qwork, vwork, spec, factor, coefs, cols_send, cols_recv, rows_send, rows_recv,
    send_sems, recv_sems, edge_send, edge_recv,
):
    count = bands * per_band
    band_me = lax.axis_index("lat")
    lon_me = lax.axis_index("lon")
    me = band_me * per_band + lon_me
    half = high_ref.shape[0]

    def place(index):
        return (index // per_band, index % per_band)

    barrier = pltpu.get_barrier_semaphore()

    def greet(i, carry):
        pl.semaphore_signal(barrier, inc=1, device_id=place((me + i) % count), device_id_type=pl.DeviceIdType.MESH)
        return carry

    lax.fori_loop(1, count, greet, 0)
    pack_edges(u_ref, v_ref, cols_send.at[0], cols_send.at[1], rows_send.at[0], rows_send.at[1])
    pl.semaphore_wait(barrier, count - 1)

    def send(source, target, sem, index):
        pltpu.make_async_remote_copy(
            src_ref=source.at[index], dst_ref=target.at[me], send_sem=send_sems.at[sem], recv_sem=recv_sems.at[sem],
            device_id=place(index), device_id_type=pl.DeviceIdType.MESH,
        ).start()

    def scatter(source, target, sem):
        def one(i, carry):
            send(source, target, sem, (me + i) % count)
            return carry

        lax.fori_loop(1, count, one, 0)
        target[me] = source[me]

    def gathered(target, sem):
        block = target.at[pl.ds(0, count - 1)]
        pltpu.make_async_copy(block, block, recv_sems.at[sem]).wait()

    def sent(source, sem):
        block = source.at[pl.ds(0, count - 1)]
        pltpu.make_async_copy(block, block, send_sems.at[sem]).wait()

    scatter(p_ref, x1, 0)

    coef_copies = []
    for i in range(1, bands):
        coef_copies.append(pltpu.make_async_remote_copy(
            src_ref=own_ref, dst_ref=coefs.at[band_me], send_sem=send_sems.at[5 + i], recv_sem=recv_sems.at[5 + i],
            device_id=((band_me + i) % bands, lon_me), device_id_type=pl.DeviceIdType.MESH,
        ))
    for copy in coef_copies:
        copy.start()
    coefs[band_me] = own_ref[...]
    edge_copies = []
    for side, step in ((0, -1), (1, 1)):
        edge_copies.append(pltpu.make_async_remote_copy(
            src_ref=cols_send.at[side], dst_ref=cols_recv.at[side], send_sem=edge_send.at[side], recv_sem=edge_recv.at[side],
            device_id=(band_me, (lon_me + per_band + step) % per_band), device_id_type=pl.DeviceIdType.MESH,
        ))
        edge_copies.append(pltpu.make_async_remote_copy(
            src_ref=rows_send.at[side], dst_ref=rows_recv.at[side], send_sem=edge_send.at[2 + side], recv_sem=edge_recv.at[2 + side],
            device_id=((band_me + bands + step) % bands, lon_me), device_id_type=pl.DeviceIdType.MESH,
        ))
    for copy in edge_copies:
        copy.start()

    limit = limit_ref[:, 0:1]
    for t in range(half):
        wave = rows_ref[t, 0:1, :]
        quotient = limit / jnp.maximum(wave, 1.0)
        factor[t] = jnp.where(wave > limit, quotient * quotient, 1.0) * rows_ref[t, 2:3, :]

    for copy in coef_copies:
        copy.wait_recv()
    gathered(x1, 0)
    to_spectrum(x1, high_ref, rest_ref, work, spec, bands, per_band, False)
    for t in range(half):
        _, _, d_part = spectral_terms(spec[t], factor[t], rows_ref[t, 1:2, :], coefs)
        work[t] = three_products(d_part, high_ref[t], rest_ref[t], True).reshape(work.shape[1:])

    def first_back(band, carry):
        put_blocks(ds1, circle_blocks(work, band), band, per_band)
        return carry

    lax.fori_loop(0, bands, first_back, 0)
    scatter(ds1, d1, 1)

    factor_columns(a_ref, s_ref, ratio, inv)
    for copy in edge_copies:
        copy.wait_recv()
    base_divergence(
        u_ref, v_ref, own_ref, cols_recv.at[1], cols_recv.at[0], rows_recv.at[1], rows_recv.at[0], base,
        band_me == 0, band_me == bands - 1,
    )
    gathered(d1, 1)
    solve_columns(a_ref, s_ref, w_ref, p_ref, base, d1, ratio, inv, w_mid, p_mid)
    scatter(p_mid, x2, 2)
    gathered(x2, 2)
    to_spectrum(x2, high_ref, rest_ref, work, spec, bands, per_band, True)
    lats = spec.shape[1]
    for t in range(half):
        smooth, v_part, d_part = spectral_terms(spec[t], factor[t], rows_ref[t, 1:2, :], coefs)
        value = three_products(jnp.concatenate([d_part, smooth, v_part], axis=0), high_ref[t], rest_ref[t], True)
        work[t] = value[:lats].reshape(work.shape[1:])
        qwork[t] = value[lats:2 * lats].reshape(work.shape[1:])
        vwork[t] = value[2 * lats:].reshape(work.shape[1:])

    def second_back(band, carry):
        put_blocks(ds2, circle_blocks(work, band), band, per_band)
        return carry

    lax.fori_loop(0, bands, second_back, 0)
    scatter(ds2, d2, 3)

    def winds_back(band, carry):
        put_blocks(vs, circle_blocks(vwork, band), band, per_band)
        zonal = coefs[band, 0][:, 0:1]
        moved = circle_diff(circle_blocks(qwork, band))
        put_blocks(us, [-zonal * x for x in moved], band, per_band)
        return carry

    lax.fori_loop(0, bands, winds_back, 0)
    scatter(us, ur, 4)
    scatter(vs, vr, 5)
    gathered(d2, 3)
    solve_columns(a_ref, s_ref, w_mid, p_mid, base, d2, ratio, inv, w_out, p_out)
    gathered(ur, 4)
    u_out[...] = u_ref[...] + ur[...]
    gathered(vr, 5)
    v_out[...] = v_ref[...] + vr[...]
    for source, sem in ((p_ref, 0), (ds1, 1), (p_mid, 2), (ds2, 3), (us, 4), (vs, 5)):
        sent(source, sem)
    for copy in coef_copies + edge_copies:
        copy.wait_send()


def level_body(
    tables,
    zonal_wind,
    merid_wind,
    vertical_wind,
    pressure,
    zonal_coef,
    merid_coef,
    level_coef,
    sound_coef,
    cutoff,
    filter_mask,
):
    high, rest, rows = (jnp.asarray(t) for t in tables)
    half = high.shape[0]
    length = half * TILE
    bands = lax.axis_size("lat")
    per_band = lax.axis_size("lon")
    lats = cutoff.shape[0]
    levels, lat_rows, width = pressure.shape
    own = jnp.broadcast_to(jnp.stack([zonal_coef, merid_coef])[:, :, None], (2, lat_rows, LANE))
    limit = jnp.where(filter_mask > 0, cutoff, length).astype(jnp.float32)
    limit = jnp.broadcast_to(limit[:, None], (lats, LANE))
    vmem = pl.BlockSpec(memory_space=pltpu.VMEM)
    smem = pl.BlockSpec(memory_space=pltpu.SMEM)
    block = jax.ShapeDtypeStruct(pressure.shape, jnp.float32)

    def scratch(*shape):
        return pltpu.VMEM(shape, jnp.float32)

    field = scratch(*pressure.shape)
    waves = scratch(half, bands, lat_rows, TILE)
    flat = scratch(half, lats, TILE)
    dma = pltpu.SemaphoreType.DMA
    return pl.pallas_call(
        functools.partial(fused_kernel, bands, per_band),
        out_shape=(block,) * 4,
        in_specs=[smem] + [vmem] * 10,
        out_specs=(vmem,) * 4,
        scratch_shapes=[field] * 15 + [waves] * 3 + [flat] * 2 + [
            scratch(bands, 2, lat_rows, LANE),
            scratch(2, lat_rows, LANE), scratch(2, lat_rows, LANE),
            scratch(2, levels, width), scratch(2, levels, width),
            dma((5 + bands,)), dma((5 + bands,)), dma((4,)), dma((4,)),
        ],
        compiler_params=pltpu.CompilerParams(collective_id=0, has_side_effects=True),
    )(level_coef, zonal_wind, merid_wind, vertical_wind, pressure, sound_coef, own, limit, high, rest, rows)


def body(tables, *arrays):
    pressure = arrays[3]
    devices = lax.axis_size("lat") * lax.axis_size("lon")
    fits = pressure.shape[0] == devices and pressure.shape[0] <= LANE and pressure.shape[1] % 8 == 0 and pressure.shape[2] % LANE == 0
    if fits:
        return level_body(tables, *arrays)
    return wide_body(*arrays)


def solution(mesh):
    in_specs = (
        P(None, "lat", "lon"),
        P(None, "lat", "lon"),
        P(None, "lat", "lon"),
        P(None, "lat", "lon"),
        P("lat"),
        P("lat"),
        P(),
        P(None, "lat", "lon"),
        P(),
        P(),
    )
    out_specs = (
        P(None, "lat", "lon"),
        P(None, "lat", "lon"),
        P(None, "lat", "lon"),
        P(None, "lat", "lon"),
    )

    def whole(*arrays):
        tables = circle_tables(arrays[0].shape[2])
        step = jax.shard_map(functools.partial(body, tables), mesh=mesh, in_specs=in_specs, out_specs=out_specs, check_vma=False)
        return step(*arrays)

    return whole
```

```python
import functools
import math

import ml_dtypes
import numpy as np
import jax
import jax.numpy as jnp
from jax import lax
from jax.experimental import pallas as pl
from jax.experimental.pallas import tpu as pltpu
from jax.sharding import PartitionSpec as P

SUBSTEPS = 2


def extended(block, sides, width):
    for axis, dim in sides:
        count = lax.axis_size(axis)
        forward = [(i, i + 1) for i in range(count - 1)]
        forward.append((count - 1, 0))
        backward = [(target, source) for source, target in forward]
        low = lax.ppermute(
            lax.slice_in_dim(block, block.shape[dim] - width, None, axis=dim), axis, forward
        )
        high = lax.ppermute(lax.slice_in_dim(block, 0, width, axis=dim), axis, backward)
        block = jnp.concatenate([low, block, high], axis=dim)
    return block


def rim_fix(padded, lat_dim):
    band_index = lax.axis_index("lat")
    bands = lax.axis_size("lat")
    extent = padded.shape[lat_dim]
    position = lax.broadcasted_iota(jnp.int32, padded.shape, lat_dim)
    first_edge = jnp.logical_and(position == 0, band_index == 0)
    final_edge = jnp.logical_and(position == extent - 1, band_index == bands - 1)
    return jnp.where(jnp.logical_or(first_edge, final_edge), 0.0, padded)


def dft_tables(length):
    half_len = length // 2
    sample = lax.broadcasted_iota(jnp.int32, (length, length), 0)
    column = lax.broadcasted_iota(jnp.int32, (length, length), 1)
    is_cosine = column <= half_len
    wavenum = jnp.where(is_cosine, column, column - half_len)
    phase = sample * wavenum % length
    angle = 2.0 * math.pi / length * phase.astype(jnp.float32)
    forward = jnp.where(is_cosine, jnp.cos(angle), jnp.sin(angle))
    single = jnp.logical_and(is_cosine, jnp.logical_or(wavenum == 0, wavenum == half_len))
    weight = jnp.where(single, 1.0, 2.0) / length
    inverse = jnp.transpose(forward * weight)
    wave_row = wavenum[0].astype(jnp.float32)
    return (forward, inverse, wave_row)


def damping(wave_row, limits):
    bound_col = limits[:, None]
    ratio = bound_col / jnp.maximum(wave_row[None, :], 1.0)
    return jnp.where(wave_row[None, :] > bound_col, ratio * ratio, 1.0)


def transform_band(block, limits, forward, inverse, wave_row):
    circles = lax.all_to_all(block, "lon", split_axis=1, concat_axis=3, tiled=True)
    spectra = jnp.einsum("vetj,jc->vetc", circles, forward, precision=lax.Precision.HIGHEST)
    scaled = spectra * damping(wave_row, limits)
    damped = jnp.einsum("vetc,cj->vetj", scaled, inverse, precision=lax.Precision.HIGHEST)
    return lax.all_to_all(damped, "lon", split_axis=3, concat_axis=1, tiled=True)


def filtered_increments(increments, own_flags, own_limits, forward, inverse, wave_row):
    flag_cols = own_flags[:, None]
    damped = transform_band(increments, own_limits, forward, inverse, wave_row)
    return jnp.where(flag_cols, damped, increments)


def column_solve(vertical_wind, pstar, level_coef, sound_coef):
    levels = vertical_wind.shape[0]
    zero_slab = jnp.zeros_like(vertical_wind[0])
    ratios = []
    values = []
    prev_ratio = zero_slab
    prev_value = zero_slab
    for level in range(levels):
        alpha = level_coef[level]
        below = alpha * sound_coef[level]
        if level + 1 < levels:
            above = alpha * sound_coef[level + 1]
            rhs = vertical_wind[level] - alpha * (pstar[level + 1] - pstar[level])
        else:
            above = zero_slab
            rhs = vertical_wind[level] + alpha * pstar[level]
        pivot = 1.0 + below + above + below * prev_ratio
        prev_ratio = -above / pivot
        prev_value = (rhs + below * prev_value) / pivot
        ratios.append(prev_ratio)
        values.append(prev_value)
    solved = [zero_slab] * levels
    upper_value = values[levels - 1]
    solved[levels - 1] = upper_value
    for level in range(levels - 2, -1, -1):
        upper_value = values[level] - ratios[level] * upper_value
        solved[level] = upper_value
    new_wind = jnp.stack(solved)
    wind_below = jnp.concatenate([zero_slab[None], new_wind[:-1]], axis=0)
    new_pressure = pstar - sound_coef * (new_wind - wind_below)
    return (new_wind, new_pressure)


def wide_body(
    zonal_wind,
    merid_wind,
    vertical_wind,
    pressure,
    zonal_coef,
    merid_coef,
    level_coef,
    sound_coef,
    cutoff,
    filter_mask,
):
    lat_rows = pressure.shape[1]
    start = lax.axis_index("lat") * lat_rows
    own_flags = lax.dynamic_slice_in_dim(filter_mask, start, lat_rows) > 0
    own_limits = lax.dynamic_slice_in_dim(cutoff, start, lat_rows).astype(jnp.float32)
    forward, inverse, wave_row = dft_tables(pressure.shape[2] * lax.axis_size("lon"))
    zonal_rows = zonal_coef[None, :, None]
    merid_rows = merid_coef[None, :, None]
    for step in range(SUBSTEPS):
        padded = extended(pressure, (("lat", 1), ("lon", 2)), 1)
        padded = rim_fix(padded, 1)
        zonal_step = -zonal_rows * (padded[:, 1:-1, 2:] - padded[:, 1:-1, :-2])
        merid_step = -merid_rows * (padded[:, 2:, 1:-1] - padded[:, :-2, 1:-1])
        increments = jnp.stack([zonal_step, merid_step])
        damped = filtered_increments(increments, own_flags, own_limits, forward, inverse, wave_row)
        winds = jnp.stack([zonal_wind, merid_wind]) + damped
        wind_pad = extended(winds, (("lat", 2), ("lon", 3)), 1)
        wind_pad = rim_fix(wind_pad, 2)
        diverge = zonal_rows * (wind_pad[0, :, 1:-1, 2:] - wind_pad[0, :, 1:-1, :-2])
        diverge = diverge + merid_rows * (wind_pad[1, :, 2:, 1:-1] - wind_pad[1, :, :-2, 1:-1])
        pstar = pressure - sound_coef * diverge
        vertical_wind, pressure = column_solve(vertical_wind, pstar, level_coef, sound_coef)
        zonal_wind = winds[0]
        merid_wind = winds[1]
    return (zonal_wind, merid_wind, vertical_wind, pressure)


LANE = 128
TILE = 2 * LANE


def circle_tables(length):
    blocks = length // LANE
    half = blocks // 2
    m = np.arange(LANE, dtype=np.float64)[:, None]
    tables = np.zeros((half, TILE, TILE))
    waves = np.zeros((half, TILE))
    c = np.arange(LANE)[None, :]
    low = np.where(c <= LANE // 2, np.cos(2 * np.pi * m * c / LANE), np.sin(2 * np.pi * m * (c - LANE // 2) / LANE))
    low = low * np.where((c == 0) | (c == LANE // 2), np.sqrt(1.0 / LANE), np.sqrt(2.0 / LANE))
    k2 = np.arange(LANE // 2)[None, :]
    angle = 2 * np.pi * m * (half + blocks * k2) / length
    mid = np.concatenate([np.cos(angle), np.sin(angle)], axis=1) * np.sqrt(2.0 / LANE)
    tables[0, :LANE, :LANE] = low
    tables[0, LANE:, LANE:] = mid
    waves[0, :LANE] = blocks * np.where(c[0] <= LANE // 2, c[0], c[0] - LANE // 2)
    waves[0, LANE:] = np.tile(half + blocks * k2[0], 2)
    for k1 in range(1, half):
        k = k1 + blocks * c
        angle = 2 * np.pi * ((m * k) % length) / length
        cos, sin = np.cos(angle) / np.sqrt(LANE), np.sin(angle) / np.sqrt(LANE)
        tables[k1] = np.block([[cos, -sin], [sin, cos]])
        waves[k1] = np.tile(np.minimum(k[0], length - k[0]), 2)
    high = tables.astype(ml_dtypes.bfloat16)
    rest = (tables - high.astype(np.float64)).astype(ml_dtypes.bfloat16)
    scale = np.full((half, TILE), 2.0 / blocks)
    scale[0] = 1.0 / blocks
    rows = np.zeros((half, 8, TILE), np.float32)
    rows[:, 0] = waves
    rows[:, 1] = 4.0 * np.sin(2 * np.pi * waves / length) ** 2
    rows[:, 2] = scale
    return high, rest, rows


def split_parts(value):
    high = value.astype(jnp.bfloat16)
    rest = (value - high.astype(jnp.float32)).astype(jnp.bfloat16)
    return high, rest


def three_products(value, high_table, rest_table, transposed):
    high, rest = split_parts(value)
    dims = (((1,), (1 if transposed else 0,)), ((), ()))
    rows = value.shape[0]
    both = lax.dot_general(jnp.concatenate([high, rest], axis=0), high_table, dims, preferred_element_type=jnp.float32)
    corr = lax.dot_general(high, rest_table, dims, preferred_element_type=jnp.float32)
    return both[:rows] + (both[rows:] + corr)


def weighted(terms):
    total = None
    for coef, value in terms:
        if abs(coef) < 1e-12:
            continue
        if abs(abs(coef) - 1.0) < 1e-12:
            term = value
        else:
            term = abs(coef) * value
        if total is None:
            total = term if coef > 0 else -term
        else:
            total = total + term if coef > 0 else total - term
    return total


def coarse_forward(xs):
    count = len(xs)
    half = count // 2
    even = {b: xs[b] + xs[count - b] for b in range(1, half)}
    odd = {b: xs[b] - xs[count - b] for b in range(1, half)}
    real, imag = [], {}
    for k in range(half + 1):
        ends = xs[0] + xs[half] if k % 2 == 0 else xs[0] - xs[half]
        real.append(weighted([(1.0, ends)] + [(math.cos(2 * math.pi * b * k / count), even[b]) for b in range(1, half)]))
    for k in range(1, half):
        imag[k] = weighted([(-math.sin(2 * math.pi * b * k / count), odd[b]) for b in range(1, half)])
    pairs = [(real[0], real[half])] + [(real[k], imag[k]) for k in range(1, half)]
    return pairs


def coarse_inverse(pairs):
    half = len(pairs)
    count = 2 * half
    first, last = pairs[0]
    xs = [None] * count
    for b in range(half + 1):
        ends = first + last if b % 2 == 0 else first - last
        cos_part = weighted([(1.0, ends)] + [(math.cos(2 * math.pi * b * k / count), pairs[k][0]) for k in range(1, half)])
        if b in (0, half):
            xs[b] = cos_part
        else:
            sin_part = weighted([(-math.sin(2 * math.pi * b * k / count), pairs[k][1]) for k in range(1, half)])
            xs[b] = cos_part + sin_part
            xs[count - b] = cos_part - sin_part
    return xs


def to_spectrum(x_ref, high_ref, rest_ref, work_ref, spec_ref, units, per_band, accumulate):
    split = x_ref.shape[2] // LANE

    def one_unit(unit, carry):
        xs = [
            x_ref[d * units + unit, :, h * LANE:(h + 1) * LANE]
            for d in range(per_band)
            for h in range(split)
        ]
        for t, (left, right) in enumerate(coarse_forward(xs)):
            work_ref[t, unit, :, :LANE] = left
            work_ref[t, unit, :, LANE:] = right
        return carry

    lax.fori_loop(0, units, one_unit, 0)
    for t in range(high_ref.shape[0]):
        value = three_products(joined(work_ref[t]), high_ref[t], rest_ref[t], False)
        if accumulate:
            value = value + spec_ref[t]
        spec_ref[t] = value


def joined(value):
    return value.reshape((value.shape[0] * value.shape[1], value.shape[2]))


def circle_blocks(work_ref, band):
    pairs = [(work_ref[t, band, :, :LANE], work_ref[t, band, :, LANE:]) for t in range(work_ref.shape[0])]
    return coarse_inverse(pairs)


def put_blocks(out_ref, xs, unit, units):
    split = out_ref.shape[2] // LANE
    for b, value in enumerate(xs):
        out_ref[(b // split) * units + unit, :, (b % split) * LANE:(b % split + 1) * LANE] = value


def circle_diff(xs):
    count = len(xs)
    lane = lax.broadcasted_iota(jnp.int32, xs[0].shape, 1)
    ahead = [pltpu.roll(x, LANE - 1, 1) for x in xs]
    behind = [pltpu.roll(x, 1, 1) for x in xs]
    out = []
    for b in range(count):
        nxt = jnp.where(lane == LANE - 1, ahead[(b + 1) % count], ahead[b])
        prv = jnp.where(lane == 0, behind[(b - 1) % count], behind[b])
        out.append(nxt - prv)
    return out


def filter_values(limit, wave, scale):
    quotient = limit / jnp.maximum(wave, 1.0)
    return jnp.where(wave > limit, quotient * quotient, 1.0) * scale


def spectral_terms(spec_ref, t, units, rows_ref, own_ref, near_ref):
    rows = own_ref.shape[1]
    wave, sines, scale = rows_ref[t, 0:1, :], rows_ref[t, 1:2, :], rows_ref[t, 2:3, :]
    zonal = own_ref[0, :, 0:1]
    merid = own_ref[1, :, 0:1]
    factor = filter_values(own_ref[2, :, 0:1], wave, scale)
    south = near_ref[0, 1, rows - 1:rows, 0:1] * filter_values(near_ref[0, 2, rows - 1:rows, 0:1], wave, scale)
    north = near_ref[1, 1, 0:1, 0:1] * filter_values(near_ref[1, 2, 0:1, 0:1], wave, scale)
    row = lax.broadcasted_iota(jnp.int32, (rows, TILE), 0)
    around = merid * factor
    along = (zonal * zonal) * sines * factor
    smooth, v_parts, d_parts = [], [], []
    for l in range(units):
        own = spec_ref[t, l * rows:(l + 1) * rows, :]
        below = spec_ref[t, units * rows + 2 * l:units * rows + 2 * l + 2, :]
        above = spec_ref[t, (units + 1) * rows + 2 * l:(units + 1) * rows + 2 * l + 2, :]
        upper = jnp.where(row == rows - 1, above[0:1], pltpu.roll(own, rows - 1, 0))
        lower = jnp.where(row == 0, below[1:2], pltpu.roll(own, 1, 0))
        mid = -around * (upper - lower)
        v_south = -south * (own[0:1] - below[0:1])
        v_north = -north * (above[1:2] - own[rows - 1:rows])
        upper = jnp.where(row == rows - 1, v_north, pltpu.roll(mid, rows - 1, 0))
        lower = jnp.where(row == 0, v_south, pltpu.roll(mid, 1, 0))
        smooth.append(factor * own)
        v_parts.append(mid)
        d_parts.append(along * own + merid * (upper - lower))
    return smooth, v_parts, d_parts


def factor_columns(a_ref, s_ref, ratio_ref, inv_ref):
    levels = s_ref.shape[0]
    prev = jnp.zeros(s_ref.shape[1:], jnp.float32)
    for level in range(levels):
        alpha = a_ref[level]
        below = alpha * s_ref[level]
        above = alpha * s_ref[level + 1] if level + 1 < levels else jnp.zeros_like(below)
        inv = 1.0 / (1.0 + below + above + below * prev)
        prev = -above * inv
        ratio_ref[level] = prev
        inv_ref[level] = inv


def solve_columns(a_ref, s_ref, w_ref, p_ref, base_ref, d_ref, ratio_ref, inv_ref, w_out, p_out):
    levels = s_ref.shape[0]

    def star(level):
        return p_ref[level] - s_ref[level] * (base_ref[level] + d_ref[level])

    here = star(0)
    prev = jnp.zeros_like(here)
    for level in range(levels):
        alpha = a_ref[level]
        p_out[level] = here
        if level + 1 < levels:
            nxt = star(level + 1)
            rhs = w_ref[level] - alpha * (nxt - here)
        else:
            nxt = here
            rhs = w_ref[level] + alpha * here
        prev = (rhs + alpha * s_ref[level] * prev) * inv_ref[level]
        w_out[level] = prev
        here = nxt
    upper = w_out[levels - 1]
    for level in range(levels - 1, 0, -1):
        lower = w_out[level - 1] - ratio_ref[level - 1] * upper
        w_out[level - 1] = lower
        p_out[level] = p_out[level] - s_ref[level] * (upper - lower)
        upper = lower
    p_out[0] = p_out[0] - s_ref[0] * upper


def base_divergence(u_ref, v_ref, own_ref, west_ref, east_ref, south_ref, north_ref, base_ref, is_first, is_last):
    zonal = own_ref[0][:, 0:1]
    merid = own_ref[1][:, 0:1]
    rows, width = u_ref.shape[1:]
    lane = lax.broadcasted_iota(jnp.int32, (rows, width), 1)
    row = lax.broadcasted_iota(jnp.int32, (rows, width), 0)
    keep_south = jnp.where(is_first, 0.0, 1.0)
    keep_north = jnp.where(is_last, 0.0, 1.0)
    west = west_ref[...]
    east = east_ref[...]
    for level in range(u_ref.shape[0]):
        u = u_ref[level]
        v = v_ref[level]
        ahead = jnp.where(lane == width - 1, east[:, level:level + 1], pltpu.roll(u, width - 1, 1))
        behind = jnp.where(lane == 0, west[:, level:level + 1], pltpu.roll(u, 1, 1))
        upper = jnp.where(row == rows - 1, keep_north * north_ref[level:level + 1, :], pltpu.roll(v, rows - 1, 0))
        lower = jnp.where(row == 0, keep_south * south_ref[level:level + 1, :], pltpu.roll(v, 1, 0))
        base_ref[level] = zonal * (ahead - behind) + merid * (upper - lower)


def pack_edges(u_ref, v_ref, first_col, last_col, first_row, last_row):
    rows, width = u_ref.shape[1:]
    lane = lax.broadcasted_iota(jnp.int32, (rows, LANE), 1)
    first = jnp.zeros((rows, LANE), jnp.float32)
    last = jnp.zeros((rows, LANE), jnp.float32)
    for level in range(u_ref.shape[0]):
        first = jnp.where(lane == level, u_ref[level, :, 0:1], first)
        last = jnp.where(lane == level, u_ref[level, :, width - 1:width], last)
        first_row[level:level + 1, :] = v_ref[level, 0:1, :]
        last_row[level:level + 1, :] = v_ref[level, rows - 1:rows, :]
    first_col[...] = first
    last_col[...] = last


def pack_halo(source, low, high, units):
    rows = source.shape[1]
    for g in range(low.shape[0]):
        for l in range(units):
            low[g, 2 * l:2 * l + 2, :] = source[g * units + l, 0:2, :]
            high[g, 2 * l:2 * l + 2, :] = source[g * units + l, rows - 2:rows, :]


def own_coefs(zc_ref, mc_ref, cutoff_ref, mask_ref, own_ref, first_lat, unfiltered):
    rows = own_ref.shape[1]
    row = lax.broadcasted_iota(jnp.int32, own_ref.shape[1:], 0)
    zonal = jnp.zeros(own_ref.shape[1:], jnp.float32)
    merid = jnp.zeros(own_ref.shape[1:], jnp.float32)
    limit = jnp.zeros(own_ref.shape[1:], jnp.int32)
    for r in range(rows):
        zonal = jnp.where(row == r, zc_ref[r], zonal)
        merid = jnp.where(row == r, mc_ref[r], merid)
        filtered = mask_ref[first_lat + r]
        bound = filtered * cutoff_ref[first_lat + r] + (1 - filtered) * unfiltered
        limit = jnp.where(row == r, bound, limit)
    own_ref[0] = zonal
    own_ref[1] = merid
    own_ref[2] = limit.astype(jnp.float32)


def fused_kernel(
    bands, per_band, a_ref, zc_ref, mc_ref, cutoff_ref, mask_ref, u_ref, v_ref, w_ref, p_ref, s_ref, high_ref, rest_ref, rows_ref,
    u_out, v_out, w_out, p_out,
    d1, d2, ur, vr, ds1, ds2, us, vs, w_mid, p_mid, base, ratio, inv,
    x1, x2, wide, work, qwork, vwork, spec, own_ref, near, cols_send, cols_recv, rows_send, rows_recv, low, high,
    send_sems, recv_sems, edge_send, edge_recv, halo_send, halo_recv,
):
    count = bands * per_band
    band_me = lax.axis_index("lat")
    lon_me = lax.axis_index("lon")
    me = band_me * per_band + lon_me
    half = high_ref.shape[0]
    lat_rows = u_ref.shape[1]
    units = u_ref.shape[0] // per_band
    spread = units + 2
    mesh_id = pl.DeviceIdType.MESH
    is_first = band_me == 0
    is_last = band_me == bands - 1

    barrier = pltpu.get_barrier_semaphore()

    def greet(i, carry):
        other = (me + i) % count
        pl.semaphore_signal(barrier, inc=1, device_id=(other // per_band, other % per_band), device_id_type=mesh_id)
        return carry

    lax.fori_loop(1, count, greet, 0)
    own_coefs(zc_ref, mc_ref, cutoff_ref, mask_ref, own_ref, band_me * lat_rows, half * TILE)
    pack_halo(p_ref, low.at[0], high.at[0], units)
    pack_edges(u_ref, v_ref, cols_send.at[0], cols_send.at[1], rows_send.at[0], rows_send.at[1])

    @pl.when(is_first)
    def _():
        near[0] = jnp.zeros(near.shape[1:], jnp.float32)
        for d in range(per_band):
            x1[d * spread + units] = jnp.zeros(x1.shape[1:], jnp.float32)
            x2[d * spread + units] = jnp.zeros(x2.shape[1:], jnp.float32)

    @pl.when(is_last)
    def _():
        near[1] = jnp.zeros(near.shape[1:], jnp.float32)
        for d in range(per_band):
            x1[d * spread + units + 1] = jnp.zeros(x1.shape[1:], jnp.float32)
            x2[d * spread + units + 1] = jnp.zeros(x2.shape[1:], jnp.float32)

    pl.semaphore_wait(barrier, count - 1)

    def scatter(source, target, sem, stride):
        def one(i, carry):
            g = (lon_me + i) % per_band
            pltpu.make_async_remote_copy(
                src_ref=source.at[pl.ds(g * units, units)], dst_ref=target.at[pl.ds(lon_me * stride, units)],
                send_sem=send_sems.at[sem], recv_sem=recv_sems.at[sem],
                device_id=(band_me, g), device_id_type=mesh_id,
            ).start()
            return carry

        lax.fori_loop(1, per_band, one, 0)
        for l in range(units):
            target[lon_me * stride + l] = source[lon_me * units + l]

    def gathered(target, sem):
        block = target.at[pl.ds(0, (per_band - 1) * units)]
        pltpu.make_async_copy(block, block, recv_sems.at[sem]).wait()

    def sent(source, sem):
        block = source.at[pl.ds(0, (per_band - 1) * units)]
        pltpu.make_async_copy(block, block, send_sems.at[sem]).wait()

    def spread_halo(target, phase):
        def one(source, slot, sem, other):
            def step(i, carry):
                g = (lon_me + i) % per_band
                pltpu.make_async_remote_copy(
                    src_ref=source.at[g], dst_ref=target.at[lon_me * spread + slot],
                    send_sem=halo_send.at[sem], recv_sem=halo_recv.at[sem],
                    device_id=(other, g), device_id_type=mesh_id,
                ).start()
                return carry

            lax.fori_loop(0, per_band, step, 0)

        @pl.when(jnp.logical_not(is_first))
        def _():
            one(low.at[phase], units + 1, 2 * phase, band_me - 1)

        @pl.when(jnp.logical_not(is_last))
        def _():
            one(high.at[phase], units, 2 * phase + 1, band_me + 1)

    def halo_wait(phase, sems, upward):
        block = low.at[phase]

        @pl.when(jnp.logical_not(is_first))
        def _():
            pltpu.make_async_copy(block, block, sems.at[2 * phase + (0 if upward else 1)]).wait()

        @pl.when(jnp.logical_not(is_last))
        def _():
            pltpu.make_async_copy(block, block, sems.at[2 * phase + (1 if upward else 0)]).wait()

    def coef_copy(step, side):
        return pltpu.make_async_remote_copy(
            src_ref=own_ref, dst_ref=near.at[side], send_sem=edge_send.at[4 + side], recv_sem=edge_recv.at[4 + side],
            device_id=((band_me + bands + step) % bands, lon_me), device_id_type=mesh_id,
        )

    @pl.when(jnp.logical_not(is_first))
    def _():
        coef_copy(-1, 1).start()

    @pl.when(jnp.logical_not(is_last))
    def _():
        coef_copy(1, 0).start()

    scatter(p_ref, x1, 0, spread)
    spread_halo(x1, 0)

    edge_copies = []
    for side, step in ((0, -1), (1, 1)):
        edge_copies.append(pltpu.make_async_remote_copy(
            src_ref=cols_send.at[side], dst_ref=cols_recv.at[side], send_sem=edge_send.at[side], recv_sem=edge_recv.at[side],
            device_id=(band_me, (lon_me + per_band + step) % per_band), device_id_type=mesh_id,
        ))
        edge_copies.append(pltpu.make_async_remote_copy(
            src_ref=rows_send.at[side], dst_ref=rows_recv.at[side], send_sem=edge_send.at[2 + side], recv_sem=edge_recv.at[2 + side],
            device_id=((band_me + bands + step) % bands, lon_me), device_id_type=mesh_id,
        ))
    for copy in edge_copies:
        copy.start()

    @pl.when(jnp.logical_not(is_first))
    def _():
        coef_copy(1, 0).wait_recv()

    @pl.when(jnp.logical_not(is_last))
    def _():
        coef_copy(-1, 1).wait_recv()

    gathered(x1, 0)
    halo_wait(0, halo_recv, False)
    to_spectrum(x1, high_ref, rest_ref, wide, spec, spread, per_band, False)
    for t in range(half):
        _, _, d_parts = spectral_terms(spec, t, units, rows_ref, own_ref, near)
        d_part = jnp.concatenate(d_parts, axis=0)
        work[t] = three_products(d_part, high_ref[t], rest_ref[t], True).reshape(work.shape[1:])

    def first_back(unit, carry):
        put_blocks(ds1, circle_blocks(work, unit), unit, units)
        return carry

    lax.fori_loop(0, units, first_back, 0)
    scatter(ds1, d1, 1, units)

    factor_columns(a_ref, s_ref, ratio, inv)
    for copy in edge_copies:
        copy.wait_recv()
    base_divergence(
        u_ref, v_ref, own_ref, cols_recv.at[1], cols_recv.at[0], rows_recv.at[1], rows_recv.at[0], base,
        is_first, is_last,
    )
    gathered(d1, 1)
    solve_columns(a_ref, s_ref, w_ref, p_ref, base, d1, ratio, inv, w_mid, p_mid)
    scatter(p_mid, x2, 2, spread)
    pack_halo(p_mid, low.at[1], high.at[1], units)
    spread_halo(x2, 1)
    gathered(x2, 2)
    halo_wait(1, halo_recv, False)
    to_spectrum(x2, high_ref, rest_ref, wide, spec, spread, per_band, True)
    lats = units * lat_rows
    for t in range(half):
        smooth, v_parts, d_parts = spectral_terms(spec, t, units, rows_ref, own_ref, near)
        value = three_products(jnp.concatenate(d_parts + smooth + v_parts, axis=0), high_ref[t], rest_ref[t], True)
        work[t] = value[:lats].reshape(work.shape[1:])
        qwork[t] = value[lats:2 * lats].reshape(work.shape[1:])
        vwork[t] = value[2 * lats:].reshape(work.shape[1:])

    def second_back(band, carry):
        put_blocks(ds2, circle_blocks(work, band), band, units)
        return carry

    lax.fori_loop(0, units, second_back, 0)
    scatter(ds2, d2, 3, units)

    def winds_back(band, carry):
        put_blocks(vs, circle_blocks(vwork, band), band, units)
        zonal = own_ref[0, :, 0:1]
        moved = circle_diff(circle_blocks(qwork, band))
        put_blocks(us, [-zonal * x for x in moved], band, units)
        return carry

    lax.fori_loop(0, units, winds_back, 0)
    scatter(us, ur, 4, units)
    scatter(vs, vr, 5, units)
    gathered(d2, 3)
    solve_columns(a_ref, s_ref, w_mid, p_mid, base, d2, ratio, inv, w_out, p_out)
    gathered(ur, 4)
    u_out[...] = u_ref[...] + ur[...]
    gathered(vr, 5)
    v_out[...] = v_ref[...] + vr[...]
    for source, sem in ((p_ref, 0), (ds1, 1), (p_mid, 2), (ds2, 3), (us, 4), (vs, 5)):
        sent(source, sem)
    for phase in range(2):
        halo_wait(phase, halo_send, True)
    for copy in edge_copies:
        copy.wait_send()

    @pl.when(jnp.logical_not(is_first))
    def _():
        coef_copy(-1, 1).wait_send()

    @pl.when(jnp.logical_not(is_last))
    def _():
        coef_copy(1, 0).wait_send()


def level_body(
    tables,
    zonal_wind,
    merid_wind,
    vertical_wind,
    pressure,
    zonal_coef,
    merid_coef,
    level_coef,
    sound_coef,
    cutoff,
    filter_mask,
):
    high, rest, rows = (jnp.asarray(t) for t in tables)
    half = high.shape[0]
    bands = lax.axis_size("lat")
    per_band = lax.axis_size("lon")
    levels, lat_rows, width = pressure.shape
    units = levels // per_band
    spread = units + 2
    vmem = pl.BlockSpec(memory_space=pltpu.VMEM)
    smem = pl.BlockSpec(memory_space=pltpu.SMEM)
    block = jax.ShapeDtypeStruct(pressure.shape, jnp.float32)

    def scratch(*shape):
        return pltpu.VMEM(shape, jnp.float32)

    field = scratch(*pressure.shape)
    arrivals = scratch(per_band * spread, lat_rows, width)
    waves = scratch(half, units, lat_rows, TILE)
    dma = pltpu.SemaphoreType.DMA
    return pl.pallas_call(
        functools.partial(fused_kernel, bands, per_band),
        out_shape=(block,) * 4,
        in_specs=[smem] * 5 + [vmem] * 8,
        out_specs=(vmem,) * 4,
        scratch_shapes=[field] * 13 + [arrivals] * 2 + [scratch(half, spread, lat_rows, TILE)] + [waves] * 3 + [
            scratch(half, spread * lat_rows, TILE),
            scratch(3, lat_rows, LANE), scratch(2, 3, lat_rows, LANE),
            scratch(2, lat_rows, LANE), scratch(2, lat_rows, LANE),
            scratch(2, levels, width), scratch(2, levels, width),
            scratch(2, per_band, lat_rows, width), scratch(2, per_band, lat_rows, width),
            dma((6,)), dma((6,)), dma((6,)), dma((6,)), dma((4,)), dma((4,)),
        ],
        compiler_params=pltpu.CompilerParams(collective_id=0, has_side_effects=True),
    )(
        level_coef, zonal_coef, merid_coef, cutoff, filter_mask,
        zonal_wind, merid_wind, vertical_wind, pressure, sound_coef, high, rest, rows,
    )


def body(tables, *arrays):
    pressure = arrays[3]
    per_band = lax.axis_size("lon")
    levels, lat_rows, width = pressure.shape
    fits = lat_rows == 8 and levels == 4 * per_band and levels <= LANE and width % LANE == 0
    if fits:
        return level_body(tables, *arrays)
    return wide_body(*arrays)


def solution(mesh):
    in_specs = (
        P(None, "lat", "lon"),
        P(None, "lat", "lon"),
        P(None, "lat", "lon"),
        P(None, "lat", "lon"),
        P("lat"),
        P("lat"),
        P(),
        P(None, "lat", "lon"),
        P(),
        P(),
    )
    out_specs = (
        P(None, "lat", "lon"),
        P(None, "lat", "lon"),
        P(None, "lat", "lon"),
        P(None, "lat", "lon"),
    )

    def whole(*arrays):
        tables = circle_tables(arrays[0].shape[2])
        step = jax.shard_map(functools.partial(body, tables), mesh=mesh, in_specs=in_specs, out_specs=out_specs, check_vma=False)
        return step(*arrays)

    return whole
```

```python
import functools
import math

import ml_dtypes
import numpy as np
import jax
import jax.numpy as jnp
from jax import lax
from jax.experimental import pallas as pl
from jax.experimental.pallas import tpu as pltpu
from jax.sharding import PartitionSpec as P

SUBSTEPS = 2


def extended(block, sides, width):
    for axis, dim in sides:
        count = lax.axis_size(axis)
        forward = [(i, i + 1) for i in range(count - 1)]
        forward.append((count - 1, 0))
        backward = [(target, source) for source, target in forward]
        low = lax.ppermute(
            lax.slice_in_dim(block, block.shape[dim] - width, None, axis=dim), axis, forward
        )
        high = lax.ppermute(lax.slice_in_dim(block, 0, width, axis=dim), axis, backward)
        block = jnp.concatenate([low, block, high], axis=dim)
    return block


def rim_fix(padded, lat_dim):
    band_index = lax.axis_index("lat")
    bands = lax.axis_size("lat")
    extent = padded.shape[lat_dim]
    position = lax.broadcasted_iota(jnp.int32, padded.shape, lat_dim)
    first_edge = jnp.logical_and(position == 0, band_index == 0)
    final_edge = jnp.logical_and(position == extent - 1, band_index == bands - 1)
    return jnp.where(jnp.logical_or(first_edge, final_edge), 0.0, padded)


def dft_tables(length):
    half_len = length // 2
    sample = lax.broadcasted_iota(jnp.int32, (length, length), 0)
    column = lax.broadcasted_iota(jnp.int32, (length, length), 1)
    is_cosine = column <= half_len
    wavenum = jnp.where(is_cosine, column, column - half_len)
    phase = sample * wavenum % length
    angle = 2.0 * math.pi / length * phase.astype(jnp.float32)
    forward = jnp.where(is_cosine, jnp.cos(angle), jnp.sin(angle))
    single = jnp.logical_and(is_cosine, jnp.logical_or(wavenum == 0, wavenum == half_len))
    weight = jnp.where(single, 1.0, 2.0) / length
    inverse = jnp.transpose(forward * weight)
    wave_row = wavenum[0].astype(jnp.float32)
    return (forward, inverse, wave_row)


def damping(wave_row, limits):
    bound_col = limits[:, None]
    ratio = bound_col / jnp.maximum(wave_row[None, :], 1.0)
    return jnp.where(wave_row[None, :] > bound_col, ratio * ratio, 1.0)


def transform_band(block, limits, forward, inverse, wave_row):
    circles = lax.all_to_all(block, "lon", split_axis=1, concat_axis=3, tiled=True)
    spectra = jnp.einsum("vetj,jc->vetc", circles, forward, precision=lax.Precision.HIGHEST)
    scaled = spectra * damping(wave_row, limits)
    damped = jnp.einsum("vetc,cj->vetj", scaled, inverse, precision=lax.Precision.HIGHEST)
    return lax.all_to_all(damped, "lon", split_axis=3, concat_axis=1, tiled=True)


def filtered_increments(increments, own_flags, own_limits, forward, inverse, wave_row):
    flag_cols = own_flags[:, None]
    damped = transform_band(increments, own_limits, forward, inverse, wave_row)
    return jnp.where(flag_cols, damped, increments)


def column_solve(vertical_wind, pstar, level_coef, sound_coef):
    levels = vertical_wind.shape[0]
    zero_slab = jnp.zeros_like(vertical_wind[0])
    ratios = []
    values = []
    prev_ratio = zero_slab
    prev_value = zero_slab
    for level in range(levels):
        alpha = level_coef[level]
        below = alpha * sound_coef[level]
        if level + 1 < levels:
            above = alpha * sound_coef[level + 1]
            rhs = vertical_wind[level] - alpha * (pstar[level + 1] - pstar[level])
        else:
            above = zero_slab
            rhs = vertical_wind[level] + alpha * pstar[level]
        pivot = 1.0 + below + above + below * prev_ratio
        prev_ratio = -above / pivot
        prev_value = (rhs + below * prev_value) / pivot
        ratios.append(prev_ratio)
        values.append(prev_value)
    solved = [zero_slab] * levels
    upper_value = values[levels - 1]
    solved[levels - 1] = upper_value
    for level in range(levels - 2, -1, -1):
        upper_value = values[level] - ratios[level] * upper_value
        solved[level] = upper_value
    new_wind = jnp.stack(solved)
    wind_below = jnp.concatenate([zero_slab[None], new_wind[:-1]], axis=0)
    new_pressure = pstar - sound_coef * (new_wind - wind_below)
    return (new_wind, new_pressure)


def wide_body(
    zonal_wind,
    merid_wind,
    vertical_wind,
    pressure,
    zonal_coef,
    merid_coef,
    level_coef,
    sound_coef,
    cutoff,
    filter_mask,
):
    lat_rows = pressure.shape[1]
    start = lax.axis_index("lat") * lat_rows
    own_flags = lax.dynamic_slice_in_dim(filter_mask, start, lat_rows) > 0
    own_limits = lax.dynamic_slice_in_dim(cutoff, start, lat_rows).astype(jnp.float32)
    forward, inverse, wave_row = dft_tables(pressure.shape[2] * lax.axis_size("lon"))
    zonal_rows = zonal_coef[None, :, None]
    merid_rows = merid_coef[None, :, None]
    for step in range(SUBSTEPS):
        padded = extended(pressure, (("lat", 1), ("lon", 2)), 1)
        padded = rim_fix(padded, 1)
        zonal_step = -zonal_rows * (padded[:, 1:-1, 2:] - padded[:, 1:-1, :-2])
        merid_step = -merid_rows * (padded[:, 2:, 1:-1] - padded[:, :-2, 1:-1])
        increments = jnp.stack([zonal_step, merid_step])
        damped = filtered_increments(increments, own_flags, own_limits, forward, inverse, wave_row)
        winds = jnp.stack([zonal_wind, merid_wind]) + damped
        wind_pad = extended(winds, (("lat", 2), ("lon", 3)), 1)
        wind_pad = rim_fix(wind_pad, 2)
        diverge = zonal_rows * (wind_pad[0, :, 1:-1, 2:] - wind_pad[0, :, 1:-1, :-2])
        diverge = diverge + merid_rows * (wind_pad[1, :, 2:, 1:-1] - wind_pad[1, :, :-2, 1:-1])
        pstar = pressure - sound_coef * diverge
        vertical_wind, pressure = column_solve(vertical_wind, pstar, level_coef, sound_coef)
        zonal_wind = winds[0]
        merid_wind = winds[1]
    return (zonal_wind, merid_wind, vertical_wind, pressure)


LANE = 128
TILE = 2 * LANE


def circle_tables(length):
    blocks = length // LANE
    half = blocks // 2
    m = np.arange(LANE, dtype=np.float64)[:, None]
    tables = np.zeros((half, TILE, TILE))
    waves = np.zeros((half, TILE))
    c = np.arange(LANE)[None, :]
    low = np.where(c <= LANE // 2, np.cos(2 * np.pi * m * c / LANE), np.sin(2 * np.pi * m * (c - LANE // 2) / LANE))
    low = low * np.where((c == 0) | (c == LANE // 2), np.sqrt(1.0 / LANE), np.sqrt(2.0 / LANE))
    k2 = np.arange(LANE // 2)[None, :]
    angle = 2 * np.pi * m * (half + blocks * k2) / length
    mid = np.concatenate([np.cos(angle), np.sin(angle)], axis=1) * np.sqrt(2.0 / LANE)
    tables[0, :LANE, :LANE] = low
    tables[0, LANE:, LANE:] = mid
    waves[0, :LANE] = blocks * np.where(c[0] <= LANE // 2, c[0], c[0] - LANE // 2)
    waves[0, LANE:] = np.tile(half + blocks * k2[0], 2)
    for k1 in range(1, half):
        k = k1 + blocks * c
        angle = 2 * np.pi * ((m * k) % length) / length
        cos, sin = np.cos(angle) / np.sqrt(LANE), np.sin(angle) / np.sqrt(LANE)
        tables[k1] = np.block([[cos, -sin], [sin, cos]])
        waves[k1] = np.tile(np.minimum(k[0], length - k[0]), 2)
    high = tables.astype(ml_dtypes.bfloat16)
    rest = (tables - high.astype(np.float64)).astype(ml_dtypes.bfloat16)
    scale = np.full((half, TILE), 2.0 / blocks)
    scale[0] = 1.0 / blocks
    rows = np.zeros((half, 8, TILE), np.float32)
    rows[:, 0] = waves
    rows[:, 1] = 4.0 * np.sin(2 * np.pi * waves / length) ** 2
    rows[:, 2] = scale
    return high, rest, rows


def split_parts(value):
    high = value.astype(jnp.bfloat16)
    rest = (value - high.astype(jnp.float32)).astype(jnp.bfloat16)
    return high, rest


def three_products(value, high_table, rest_table, transposed):
    high, rest = split_parts(value)
    dims = (((1,), (1 if transposed else 0,)), ((), ()))
    rows = value.shape[0]
    both = lax.dot_general(jnp.concatenate([high, rest], axis=0), high_table, dims, preferred_element_type=jnp.float32)
    corr = lax.dot_general(high, rest_table, dims, preferred_element_type=jnp.float32)
    return both[:rows] + (both[rows:] + corr)


def weighted(terms):
    total = None
    for coef, value in terms:
        if abs(coef) < 1e-12:
            continue
        if abs(abs(coef) - 1.0) < 1e-12:
            term = value
        else:
            term = abs(coef) * value
        if total is None:
            total = term if coef > 0 else -term
        else:
            total = total + term if coef > 0 else total - term
    return total


def coarse_forward(xs):
    count = len(xs)
    half = count // 2
    even = {b: xs[b] + xs[count - b] for b in range(1, half)}
    odd = {b: xs[b] - xs[count - b] for b in range(1, half)}
    real, imag = [], {}
    for k in range(half + 1):
        ends = xs[0] + xs[half] if k % 2 == 0 else xs[0] - xs[half]
        real.append(weighted([(1.0, ends)] + [(math.cos(2 * math.pi * b * k / count), even[b]) for b in range(1, half)]))
    for k in range(1, half):
        imag[k] = weighted([(-math.sin(2 * math.pi * b * k / count), odd[b]) for b in range(1, half)])
    pairs = [(real[0], real[half])] + [(real[k], imag[k]) for k in range(1, half)]
    return pairs


def coarse_inverse(pairs):
    half = len(pairs)
    count = 2 * half
    first, last = pairs[0]
    xs = [None] * count
    for b in range(half + 1):
        ends = first + last if b % 2 == 0 else first - last
        cos_part = weighted([(1.0, ends)] + [(math.cos(2 * math.pi * b * k / count), pairs[k][0]) for k in range(1, half)])
        if b in (0, half):
            xs[b] = cos_part
        else:
            sin_part = weighted([(-math.sin(2 * math.pi * b * k / count), pairs[k][1]) for k in range(1, half)])
            xs[b] = cos_part + sin_part
            xs[count - b] = cos_part - sin_part
    return xs


def to_spectrum(x_ref, high_ref, rest_ref, work_ref, spec_ref, units, per_band, accumulate):
    split = x_ref.shape[2] // LANE

    def one_unit(unit, carry):
        xs = [
            x_ref[d * units + unit, :, h * LANE:(h + 1) * LANE]
            for d in range(per_band)
            for h in range(split)
        ]
        for t, (left, right) in enumerate(coarse_forward(xs)):
            work_ref[t, unit, :, :LANE] = left
            work_ref[t, unit, :, LANE:] = right
        return carry

    lax.fori_loop(0, units, one_unit, 0)
    for t in range(high_ref.shape[0]):
        value = three_products(joined(work_ref[t]), high_ref[t], rest_ref[t], False)
        if accumulate:
            value = value + spec_ref[t]
        spec_ref[t] = value


def joined(value):
    return value.reshape((value.shape[0] * value.shape[1], value.shape[2]))


def circle_blocks(work_ref, band):
    pairs = [(work_ref[t, band, :, :LANE], work_ref[t, band, :, LANE:]) for t in range(work_ref.shape[0])]
    return coarse_inverse(pairs)


def put_blocks(out_ref, xs, unit, units):
    split = out_ref.shape[2] // LANE
    for b, value in enumerate(xs):
        out_ref[(b // split) * units + unit, :, (b % split) * LANE:(b % split + 1) * LANE] = value


def circle_diff(xs):
    count = len(xs)
    lane = lax.broadcasted_iota(jnp.int32, xs[0].shape, 1)
    ahead = [pltpu.roll(x, LANE - 1, 1) for x in xs]
    behind = [pltpu.roll(x, 1, 1) for x in xs]
    out = []
    for b in range(count):
        nxt = jnp.where(lane == LANE - 1, ahead[(b + 1) % count], ahead[b])
        prv = jnp.where(lane == 0, behind[(b - 1) % count], behind[b])
        out.append(nxt - prv)
    return out


def filter_values(limit, wave, scale):
    quotient = limit / jnp.maximum(wave, 1.0)
    return jnp.where(wave > limit, quotient * quotient, 1.0) * scale


def spectral_terms(spec_ref, t, units, rows_ref, own_ref, near_ref):
    rows = own_ref.shape[1]
    wave, sines, scale = rows_ref[t, 0:1, :], rows_ref[t, 1:2, :], rows_ref[t, 2:3, :]
    zonal = own_ref[0, :, 0:1]
    merid = own_ref[1, :, 0:1]
    factor = filter_values(own_ref[2, :, 0:1], wave, scale)
    south = near_ref[0, 1, rows - 1:rows, 0:1] * filter_values(near_ref[0, 2, rows - 1:rows, 0:1], wave, scale)
    north = near_ref[1, 1, 0:1, 0:1] * filter_values(near_ref[1, 2, 0:1, 0:1], wave, scale)
    row = lax.broadcasted_iota(jnp.int32, (rows, TILE), 0)
    around = merid * factor
    along = (zonal * zonal) * sines * factor
    smooth, v_parts, d_parts = [], [], []
    for l in range(units):
        own = spec_ref[t, l * rows:(l + 1) * rows, :]
        below = spec_ref[t, units * rows + 2 * l:units * rows + 2 * l + 2, :]
        above = spec_ref[t, (units + 1) * rows + 2 * l:(units + 1) * rows + 2 * l + 2, :]
        upper = jnp.where(row == rows - 1, above[0:1], pltpu.roll(own, rows - 1, 0))
        lower = jnp.where(row == 0, below[1:2], pltpu.roll(own, 1, 0))
        mid = -around * (upper - lower)
        v_south = -south * (own[0:1] - below[0:1])
        v_north = -north * (above[1:2] - own[rows - 1:rows])
        upper = jnp.where(row == rows - 1, v_north, pltpu.roll(mid, rows - 1, 0))
        lower = jnp.where(row == 0, v_south, pltpu.roll(mid, 1, 0))
        smooth.append(factor * own)
        v_parts.append(mid)
        d_parts.append(along * own + merid * (upper - lower))
    return smooth, v_parts, d_parts


def factor_columns(a_ref, s_ref, ratio_ref, inv_ref):
    levels = s_ref.shape[0]
    prev = jnp.zeros(s_ref.shape[1:], jnp.float32)
    for level in range(levels):
        alpha = a_ref[level]
        below = alpha * s_ref[level]
        above = alpha * s_ref[level + 1] if level + 1 < levels else jnp.zeros_like(below)
        inv = 1.0 / (1.0 + below + above + below * prev)
        prev = -above * inv
        ratio_ref[level] = prev
        inv_ref[level] = inv


def solve_columns(a_ref, s_ref, w_ref, p_ref, base_ref, d_ref, ratio_ref, inv_ref, w_out, p_out):
    levels = s_ref.shape[0]

    def star(level):
        return p_ref[level] - s_ref[level] * (base_ref[level] + d_ref[level])

    here = star(0)
    prev = jnp.zeros_like(here)
    for level in range(levels):
        alpha = a_ref[level]
        p_out[level] = here
        if level + 1 < levels:
            nxt = star(level + 1)
            rhs = w_ref[level] - alpha * (nxt - here)
        else:
            nxt = here
            rhs = w_ref[level] + alpha * here
        prev = (rhs + alpha * s_ref[level] * prev) * inv_ref[level]
        w_out[level] = prev
        here = nxt
    upper = w_out[levels - 1]
    for level in range(levels - 1, 0, -1):
        lower = w_out[level - 1] - ratio_ref[level - 1] * upper
        w_out[level - 1] = lower
        p_out[level] = p_out[level] - s_ref[level] * (upper - lower)
        upper = lower
    p_out[0] = p_out[0] - s_ref[0] * upper


def base_divergence(u_ref, v_ref, own_ref, west_ref, east_ref, south_ref, north_ref, base_ref, is_first, is_last):
    zonal = own_ref[0][:, 0:1]
    merid = own_ref[1][:, 0:1]
    rows, width = u_ref.shape[1:]
    lane = lax.broadcasted_iota(jnp.int32, (rows, width), 1)
    row = lax.broadcasted_iota(jnp.int32, (rows, width), 0)
    keep_south = jnp.where(is_first, 0.0, 1.0)
    keep_north = jnp.where(is_last, 0.0, 1.0)
    west = west_ref[...]
    east = east_ref[...]
    for level in range(u_ref.shape[0]):
        u = u_ref[level]
        v = v_ref[level]
        ahead = jnp.where(lane == width - 1, east[:, level:level + 1], pltpu.roll(u, width - 1, 1))
        behind = jnp.where(lane == 0, west[:, level:level + 1], pltpu.roll(u, 1, 1))
        upper = jnp.where(row == rows - 1, keep_north * north_ref[level:level + 1, :], pltpu.roll(v, rows - 1, 0))
        lower = jnp.where(row == 0, keep_south * south_ref[level:level + 1, :], pltpu.roll(v, 1, 0))
        base_ref[level] = zonal * (ahead - behind) + merid * (upper - lower)


def pack_edges(u_ref, v_ref, first_col, last_col, first_row, last_row):
    rows, width = u_ref.shape[1:]
    lane = lax.broadcasted_iota(jnp.int32, (rows, LANE), 1)
    first = jnp.zeros((rows, LANE), jnp.float32)
    last = jnp.zeros((rows, LANE), jnp.float32)
    for level in range(u_ref.shape[0]):
        first = jnp.where(lane == level, u_ref[level, :, 0:1], first)
        last = jnp.where(lane == level, u_ref[level, :, width - 1:width], last)
        first_row[level:level + 1, :] = v_ref[level, 0:1, :]
        last_row[level:level + 1, :] = v_ref[level, rows - 1:rows, :]
    first_col[...] = first
    last_col[...] = last


def pack_halo(source, low, high, units):
    rows = source.shape[1]
    for g in range(low.shape[0]):
        for l in range(units):
            low[g, 2 * l:2 * l + 2, :] = source[g * units + l, 0:2, :]
            high[g, 2 * l:2 * l + 2, :] = source[g * units + l, rows - 2:rows, :]


def own_coefs(zc_ref, mc_ref, cutoff_ref, mask_ref, own_ref, first_lat, unfiltered):
    rows = own_ref.shape[1]
    row = lax.broadcasted_iota(jnp.int32, own_ref.shape[1:], 0)
    zonal = jnp.zeros(own_ref.shape[1:], jnp.float32)
    merid = jnp.zeros(own_ref.shape[1:], jnp.float32)
    limit = jnp.zeros(own_ref.shape[1:], jnp.int32)
    for r in range(rows):
        zonal = jnp.where(row == r, zc_ref[r], zonal)
        merid = jnp.where(row == r, mc_ref[r], merid)
        filtered = mask_ref[first_lat + r]
        bound = filtered * cutoff_ref[first_lat + r] + (1 - filtered) * unfiltered
        limit = jnp.where(row == r, bound, limit)
    own_ref[0] = zonal
    own_ref[1] = merid
    own_ref[2] = limit.astype(jnp.float32)


def fused_kernel(
    bands, per_band, a_ref, zc_ref, mc_ref, cutoff_ref, mask_ref, u_ref, v_ref, w_far, p_ref, s_far, high_far, rest_far, rows_ref,
    u_out, v_out, w_out, p_out,
    d1, d2, ur, vr, ds1, ds2, us, vs, w_mid, p_mid, base, ratio, inv,
    x1, x2, wide, work, qwork, vwork, spec, own_ref, near, cols_send, cols_recv, rows_send, rows_recv, low, high,
    send_sems, recv_sems, edge_send, edge_recv, halo_send, halo_recv,
    w_ref, s_ref, high_ref, rest_ref, load_sems,
):
    count = bands * per_band
    band_me = lax.axis_index("lat")
    lon_me = lax.axis_index("lon")
    me = band_me * per_band + lon_me
    half = high_ref.shape[0]
    lat_rows = u_ref.shape[1]
    units = u_ref.shape[0] // per_band
    spread = units + 2
    mesh_id = pl.DeviceIdType.MESH
    is_first = band_me == 0
    is_last = band_me == bands - 1

    loads = [
        pltpu.make_async_copy(far, here, load_sems.at[n])
        for n, (far, here) in enumerate(((high_far, high_ref), (rest_far, rest_ref), (s_far, s_ref), (w_far, w_ref)))
    ]
    for load in loads:
        load.start()
    barrier = pltpu.get_barrier_semaphore()

    def greet(i, carry):
        other = (me + i) % count
        pl.semaphore_signal(barrier, inc=1, device_id=(other // per_band, other % per_band), device_id_type=mesh_id)
        return carry

    lax.fori_loop(1, count, greet, 0)
    own_coefs(zc_ref, mc_ref, cutoff_ref, mask_ref, own_ref, band_me * lat_rows, half * TILE)
    pack_halo(p_ref, low.at[0], high.at[0], units)
    pack_edges(u_ref, v_ref, cols_send.at[0], cols_send.at[1], rows_send.at[0], rows_send.at[1])

    @pl.when(is_first)
    def _():
        near[0] = jnp.zeros(near.shape[1:], jnp.float32)
        for d in range(per_band):
            x1[d * spread + units] = jnp.zeros(x1.shape[1:], jnp.float32)
            x2[d * spread + units] = jnp.zeros(x2.shape[1:], jnp.float32)

    @pl.when(is_last)
    def _():
        near[1] = jnp.zeros(near.shape[1:], jnp.float32)
        for d in range(per_band):
            x1[d * spread + units + 1] = jnp.zeros(x1.shape[1:], jnp.float32)
            x2[d * spread + units + 1] = jnp.zeros(x2.shape[1:], jnp.float32)

    pl.semaphore_wait(barrier, count - 1)

    def scatter(source, target, sem, stride):
        def one(i, carry):
            g = (lon_me + i) % per_band
            pltpu.make_async_remote_copy(
                src_ref=source.at[pl.ds(g * units, units)], dst_ref=target.at[pl.ds(lon_me * stride, units)],
                send_sem=send_sems.at[sem], recv_sem=recv_sems.at[sem],
                device_id=(band_me, g), device_id_type=mesh_id,
            ).start()
            return carry

        lax.fori_loop(1, per_band, one, 0)
        for l in range(units):
            target[lon_me * stride + l] = source[lon_me * units + l]

    def gathered(target, sem):
        block = target.at[pl.ds(0, (per_band - 1) * units)]
        pltpu.make_async_copy(block, block, recv_sems.at[sem]).wait()

    def sent(source, sem):
        block = source.at[pl.ds(0, (per_band - 1) * units)]
        pltpu.make_async_copy(block, block, send_sems.at[sem]).wait()

    def spread_halo(target, phase):
        def one(source, slot, sem, other):
            def step(i, carry):
                g = (lon_me + i) % per_band
                pltpu.make_async_remote_copy(
                    src_ref=source.at[g], dst_ref=target.at[lon_me * spread + slot],
                    send_sem=halo_send.at[sem], recv_sem=halo_recv.at[sem],
                    device_id=(other, g), device_id_type=mesh_id,
                ).start()
                return carry

            lax.fori_loop(0, per_band, step, 0)

        @pl.when(jnp.logical_not(is_first))
        def _():
            one(low.at[phase], units + 1, 2 * phase, band_me - 1)

        @pl.when(jnp.logical_not(is_last))
        def _():
            one(high.at[phase], units, 2 * phase + 1, band_me + 1)

    def halo_wait(phase, sems, upward):
        block = low.at[phase]

        @pl.when(jnp.logical_not(is_first))
        def _():
            pltpu.make_async_copy(block, block, sems.at[2 * phase + (0 if upward else 1)]).wait()

        @pl.when(jnp.logical_not(is_last))
        def _():
            pltpu.make_async_copy(block, block, sems.at[2 * phase + (1 if upward else 0)]).wait()

    def coef_copy(step, side):
        return pltpu.make_async_remote_copy(
            src_ref=own_ref, dst_ref=near.at[side], send_sem=edge_send.at[4 + side], recv_sem=edge_recv.at[4 + side],
            device_id=((band_me + bands + step) % bands, lon_me), device_id_type=mesh_id,
        )

    @pl.when(jnp.logical_not(is_first))
    def _():
        coef_copy(-1, 1).start()

    @pl.when(jnp.logical_not(is_last))
    def _():
        coef_copy(1, 0).start()

    scatter(p_ref, x1, 0, spread)
    spread_halo(x1, 0)

    edge_copies = []
    for side, step in ((0, -1), (1, 1)):
        edge_copies.append(pltpu.make_async_remote_copy(
            src_ref=cols_send.at[side], dst_ref=cols_recv.at[side], send_sem=edge_send.at[side], recv_sem=edge_recv.at[side],
            device_id=(band_me, (lon_me + per_band + step) % per_band), device_id_type=mesh_id,
        ))
        edge_copies.append(pltpu.make_async_remote_copy(
            src_ref=rows_send.at[side], dst_ref=rows_recv.at[side], send_sem=edge_send.at[2 + side], recv_sem=edge_recv.at[2 + side],
            device_id=((band_me + bands + step) % bands, lon_me), device_id_type=mesh_id,
        ))
    for copy in edge_copies:
        copy.start()

    @pl.when(jnp.logical_not(is_first))
    def _():
        coef_copy(1, 0).wait_recv()

    @pl.when(jnp.logical_not(is_last))
    def _():
        coef_copy(-1, 1).wait_recv()

    for load in loads:
        load.wait()
    gathered(x1, 0)
    halo_wait(0, halo_recv, False)
    to_spectrum(x1, high_ref, rest_ref, wide, spec, spread, per_band, False)
    for t in range(half):
        _, _, d_parts = spectral_terms(spec, t, units, rows_ref, own_ref, near)
        d_part = jnp.concatenate(d_parts, axis=0)
        work[t] = three_products(d_part, high_ref[t], rest_ref[t], True).reshape(work.shape[1:])

    def first_back(unit, carry):
        put_blocks(ds1, circle_blocks(work, unit), unit, units)
        return carry

    lax.fori_loop(0, units, first_back, 0)
    scatter(ds1, d1, 1, units)

    factor_columns(a_ref, s_ref, ratio, inv)
    for copy in edge_copies:
        copy.wait_recv()
    base_divergence(
        u_ref, v_ref, own_ref, cols_recv.at[1], cols_recv.at[0], rows_recv.at[1], rows_recv.at[0], base,
        is_first, is_last,
    )
    gathered(d1, 1)
    solve_columns(a_ref, s_ref, w_ref, p_ref, base, d1, ratio, inv, w_mid, p_mid)
    scatter(p_mid, x2, 2, spread)
    pack_halo(p_mid, low.at[1], high.at[1], units)
    spread_halo(x2, 1)
    gathered(x2, 2)
    halo_wait(1, halo_recv, False)
    to_spectrum(x2, high_ref, rest_ref, wide, spec, spread, per_band, True)
    lats = units * lat_rows
    for t in range(half):
        smooth, v_parts, d_parts = spectral_terms(spec, t, units, rows_ref, own_ref, near)
        value = three_products(jnp.concatenate(d_parts + smooth + v_parts, axis=0), high_ref[t], rest_ref[t], True)
        work[t] = value[:lats].reshape(work.shape[1:])
        qwork[t] = value[lats:2 * lats].reshape(work.shape[1:])
        vwork[t] = value[2 * lats:].reshape(work.shape[1:])

    def second_back(band, carry):
        put_blocks(ds2, circle_blocks(work, band), band, units)
        return carry

    lax.fori_loop(0, units, second_back, 0)
    scatter(ds2, d2, 3, units)

    def winds_back(band, carry):
        put_blocks(vs, circle_blocks(vwork, band), band, units)
        zonal = own_ref[0, :, 0:1]
        moved = circle_diff(circle_blocks(qwork, band))
        put_blocks(us, [-zonal * x for x in moved], band, units)
        return carry

    lax.fori_loop(0, units, winds_back, 0)
    scatter(us, ur, 4, units)
    scatter(vs, vr, 5, units)
    gathered(d2, 3)
    solve_columns(a_ref, s_ref, w_mid, p_mid, base, d2, ratio, inv, w_out, p_out)
    gathered(ur, 4)
    u_out[...] = u_ref[...] + ur[...]
    gathered(vr, 5)
    v_out[...] = v_ref[...] + vr[...]
    for source, sem in ((p_ref, 0), (ds1, 1), (p_mid, 2), (ds2, 3), (us, 4), (vs, 5)):
        sent(source, sem)
    for phase in range(2):
        halo_wait(phase, halo_send, True)
    for copy in edge_copies:
        copy.wait_send()

    @pl.when(jnp.logical_not(is_first))
    def _():
        coef_copy(-1, 1).wait_send()

    @pl.when(jnp.logical_not(is_last))
    def _():
        coef_copy(1, 0).wait_send()


def level_body(
    tables,
    zonal_wind,
    merid_wind,
    vertical_wind,
    pressure,
    zonal_coef,
    merid_coef,
    level_coef,
    sound_coef,
    cutoff,
    filter_mask,
):
    high, rest, rows = (jnp.asarray(t) for t in tables)
    half = high.shape[0]
    bands = lax.axis_size("lat")
    per_band = lax.axis_size("lon")
    levels, lat_rows, width = pressure.shape
    units = levels // per_band
    spread = units + 2
    vmem = pl.BlockSpec(memory_space=pltpu.VMEM)
    smem = pl.BlockSpec(memory_space=pltpu.SMEM)
    far = pl.BlockSpec(memory_space=pl.ANY)
    block = jax.ShapeDtypeStruct(pressure.shape, jnp.float32)

    def scratch(*shape):
        return pltpu.VMEM(shape, jnp.float32)

    field = scratch(*pressure.shape)
    arrivals = scratch(per_band * spread, lat_rows, width)
    waves = scratch(half, units, lat_rows, TILE)
    dma = pltpu.SemaphoreType.DMA
    return pl.pallas_call(
        functools.partial(fused_kernel, bands, per_band),
        out_shape=(block,) * 4,
        in_specs=[smem] * 5 + [vmem] * 2 + [far, vmem, far, far, far, vmem],
        out_specs=(vmem,) * 4,
        scratch_shapes=[field] * 13 + [arrivals] * 2 + [scratch(half, spread, lat_rows, TILE)] + [waves] * 3 + [
            scratch(half, spread * lat_rows, TILE),
            scratch(3, lat_rows, LANE), scratch(2, 3, lat_rows, LANE),
            scratch(2, lat_rows, LANE), scratch(2, lat_rows, LANE),
            scratch(2, levels, width), scratch(2, levels, width),
            scratch(2, per_band, lat_rows, width), scratch(2, per_band, lat_rows, width),
            dma((6,)), dma((6,)), dma((6,)), dma((6,)), dma((4,)), dma((4,)),
            field, field, pltpu.VMEM(high.shape, high.dtype), pltpu.VMEM(rest.shape, rest.dtype), dma((4,)),
        ],
        compiler_params=pltpu.CompilerParams(collective_id=0, has_side_effects=True),
    )(
        level_coef, zonal_coef, merid_coef, cutoff, filter_mask,
        zonal_wind, merid_wind, vertical_wind, pressure, sound_coef, high, rest, rows,
    )


def body(tables, *arrays):
    pressure = arrays[3]
    per_band = lax.axis_size("lon")
    levels, lat_rows, width = pressure.shape
    fits = lat_rows == 8 and levels == 4 * per_band and levels <= LANE and width % LANE == 0
    if fits:
        return level_body(tables, *arrays)
    return wide_body(*arrays)


def solution(mesh):
    in_specs = (
        P(None, "lat", "lon"),
        P(None, "lat", "lon"),
        P(None, "lat", "lon"),
        P(None, "lat", "lon"),
        P("lat"),
        P("lat"),
        P(),
        P(None, "lat", "lon"),
        P(),
        P(),
    )
    out_specs = (
        P(None, "lat", "lon"),
        P(None, "lat", "lon"),
        P(None, "lat", "lon"),
        P(None, "lat", "lon"),
    )

    def whole(*arrays):
        tables = circle_tables(arrays[0].shape[2])
        step = jax.shard_map(functools.partial(body, tables), mesh=mesh, in_specs=in_specs, out_specs=out_specs, check_vma=False)
        return step(*arrays)

    return whole
```
